32 devices in a mesh: groups: 2 (over x), seq: 8 (over z, y), mp: 2 (over core).
Axes of the slice: x: 2, y: 2, z: 4, core: 2. Of those that a mesh axis runs over, the one named last changes fastest.
Arguments:
- latent_cache: bfloat16 [2048, 64, 512], P(('groups', 'seq')), parts along dimension 0, may hold values from -6 to 6
- rope_cache: bfloat16 [2048, 4096], P(('groups', 'seq')), parts along dimension 0, may hold values from -6 to 6
- q_nope: bfloat16 [16, 128, 128], P('groups', 'mp'), parts along dimension 0, may hold values from -12 to 12
- q_rope: bfloat16 [16, 128, 64], P('groups', 'mp'), parts along dimension 0, may hold values from -2000 to 2000
- w_uk: bfloat16 [128, 128, 512], P('mp', None, 'seq'), may hold values from -0.5 to 0.5
- value_up_weight: bfloat16 [128, 512, 128], P('mp', 'seq'), may hold values from -0.25 to 0.25
- w_out: bfloat16 [16384, 7168], P('mp', 'seq'), may hold values from -0.046875 to 0.046875
- page_table: int32 [16, 256], P('groups'), parts along dimension 0, may hold values from 0 to 1023, as said below
- lengths: int32 [16], P('groups'), parts along dimension 0, may hold values from 2048 to 16384, as said below
Outputs:
- output: bfloat16 [16, 7168], P('groups', ('seq', 'mp')), parts along dimension 0
The draws below stay inside these ranges and needn't reach their ends.
There are 2 independent parts, one for each index of `groups`. The reference program is written for one: setup_inputs(seed, part) draws one part's arguments, and reference() takes and returns one part's arrays. A program takes and returns all parts, laid end to end along the dimension named above; an argument that names none is the same for every part. Nothing has to cross between parts.
Inputs may be any that keep to these rules, and one draw needn't show every extreme that they name: `lengths`: every sequence has one eighth of 16384 tokens or more; the longest has exactly 16384. page_table[b,p] for p < ceil(lengths[b] / 64) is the global slot (shard index times 128 plus local slot) holding that page; these live entries are all distinct; the other entries are 0 and unused.
All inputs are finite; a program needn't handle non-finite values.
Results may differ from the reference program's by a relative error of at most 0.012.
Values may be sent and summed in bfloat16 or wider, within the bound.
A program may use at most 128 MiB of HBM per device.

```python
import jax
import jax.numpy as jnp
from jax import lax

B = 8
H = 128
NOPE = 128
ROPE = 64
KVR = 512
VDIM = 128
D = 7168
PAGE = 64
SLOTS_DEV = 128
SLOTS = 1024
MAXLEN = 16384
MAXPAGES = 256
N_SEQ = 8


def page_layout(key):
    key_len, key_long, key_weight, key_perm = jax.random.split(jax.random.fold_in(key, 11), 4)
    others = jax.random.randint(key_len, (B,), MAXLEN // 8, MAXLEN // 4 + 1)
    longest_length = jax.random.randint(key_long, (), 0, B)
    lengths = jnp.where(jnp.arange(B) == longest_length, MAXLEN, others).astype(jnp.int32)
    page_count = (lengths + PAGE - 1) // PAGE
    offsets = jnp.cumsum(page_count) - page_count
    weight = jax.random.randint(key_weight, (N_SEQ,), 0, 4)
    shuffled = jax.random.permutation(key_perm, SLOTS)
    ranking = jnp.repeat(weight, SLOTS_DEV) * SLOTS + shuffled
    slot_order = jnp.argsort(-ranking)
    logical = jnp.arange(MAXPAGES)
    position = jnp.clip(offsets[:, None] + logical[None, :], 0, SLOTS - 1)
    page_map = jnp.where(logical[None, :] < page_count[:, None], slot_order[position], 0).astype(jnp.int32)
    return (lengths, page_map)


def rope_values(key):
    base = jnp.clip(jax.random.normal(jax.random.fold_in(key, 23), (SLOTS, PAGE, ROPE), jnp.float32), -6.0, 6.0)
    return base


def draw_lengths(key, part):
    return page_layout(key)[0]


def draw_page_table(key, part):
    return page_layout(key)[1]


def draw_rope_cache(key, part):
    return rope_values(key).reshape(SLOTS, PAGE * ROPE).astype(jnp.bfloat16)


def draw_q_rope(key, part):
    drawn = jnp.clip(2.0 * jax.random.normal(jax.random.fold_in(key, 31), (B, H, ROPE), jnp.float32), -12.0, 12.0)
    return drawn.astype(jnp.bfloat16)


def steps_of(key, dims, shards, low, high):
    gain, own = 1.0, jax.random.fold_in(key, 6)
    for dim, blocks in shards:
        steps = jnp.exp(jax.random.uniform(jax.random.fold_in(own, dim), (blocks,), jnp.float32, low / len(shards), high / len(shards)))
        gain = gain * jnp.repeat(steps, dims[dim] // blocks).reshape([-1 if axis == dim else 1 for axis in range(len(dims))])
    return gain


def gaussian(rng, extent, deviation, limit, cuts=(), held_as=jnp.bfloat16):
    gain = steps_of(rng, extent, cuts, -0.22, 0.18) if cuts else 1.0
    values = jax.random.normal(rng, extent, jnp.float32) * deviation * gain
    return jnp.minimum(jnp.maximum(values, -limit), limit).astype(held_as)


def setup_inputs(seed: int = 0, part: int = 0) -> dict:
    splits = jax.random.split(jax.random.key(seed), 10)
    part_keys = jax.random.split(jax.random.fold_in(splits[9], part), 10)
    latent_cache = gaussian(part_keys[0], (SLOTS, PAGE, KVR), 1.0, 6.0, ((0, 8),))
    rope_cache = draw_rope_cache(jax.random.fold_in(jax.random.fold_in(splits[9], part), 71), part)
    q_nope = gaussian(part_keys[2], (B, H, NOPE), 2.0, 12.0, ((1, 2),))
    q_rope = draw_q_rope(jax.random.fold_in(jax.random.fold_in(splits[9], part), 71), part)
    w_uk = gaussian(splits[4], (H, NOPE, KVR), NOPE ** -0.5, 0.5, ((0, 2), (2, 8)))
    value_up_weight = gaussian(splits[5], (H, KVR, VDIM), KVR ** -0.5, 0.25, ((0, 2), (1, 8)))
    w_out = gaussian(splits[6], (H * VDIM, D), (H * VDIM) ** -0.5, 0.046875, ((0, 2), (1, 8)))
    page_table = draw_page_table(jax.random.fold_in(jax.random.fold_in(splits[9], part), 71), part)
    lengths = draw_lengths(jax.random.fold_in(jax.random.fold_in(splits[9], part), 71), part)
    return dict(latent_cache=latent_cache, rope_cache=rope_cache, q_nope=q_nope, q_rope=q_rope, w_uk=w_uk, value_up_weight=value_up_weight, w_out=w_out, page_table=page_table, lengths=lengths)


NEG = -1.0e30


def reference(latent_cache, rope_cache, q_nope, q_rope, w_uk, value_up_weight, w_out, page_table, lengths):
    score_scale = (NOPE + ROPE) ** -0.5
    peak_score = lax.Precision.HIGHEST
    q_latent = jnp.einsum('bhn,hnk->bhk', q_nope.astype(jnp.float32), w_uk.astype(jnp.float32), precision=peak_score).astype(jnp.bfloat16)
    page_count = (lengths + PAGE - 1) // PAGE
    logical = jnp.arange(MAXPAGES, dtype=jnp.int32)
    live_page = logical[None, :] < page_count[:, None]
    tokens_in = jnp.clip(lengths[:, None] - PAGE * logical[None, :], 0, PAGE).astype(jnp.int32)
    target = jnp.where(live_page, page_table, SLOTS).astype(jnp.int32).reshape(-1)
    seq_ids = jnp.broadcast_to(jnp.arange(B, dtype=jnp.int32)[:, None], (B, MAXPAGES)).reshape(-1)
    slot_owner = jnp.zeros((SLOTS, B), jnp.float32).at[target, seq_ids].set(1.0, mode='drop')
    slot_fill = jnp.zeros((SLOTS,), jnp.int32).at[target].add(tokens_in.reshape(-1), mode='drop')
    blocks = SLOTS // 8
    latent_blocks = latent_cache.reshape(blocks, 8, PAGE, KVR)
    rope_blocks = rope_cache.reshape(blocks, 8, PAGE, ROPE)
    owner_blocks = slot_owner.reshape(blocks, 8, B)
    fill_blocks = slot_fill.reshape(blocks, 8)
    q_latent_f = q_latent.astype(jnp.float32)
    q_rope_f = q_rope.astype(jnp.float32)

    def step_block(run_state, block_data):
        run_max, run_sum, run_out = run_state
        latent_block, rope_block, owner_block, fill_block = block_data
        latent_f = latent_block.astype(jnp.float32)
        pick_latent = jnp.einsum('sb,bhk->shk', owner_block, q_latent_f, precision=peak_score)
        pick_rope = jnp.einsum('sb,bhr->shr', owner_block, q_rope_f, precision=peak_score)
        scores = (jnp.einsum('shk,stk->sht', pick_latent, latent_f, precision=peak_score)
                  + jnp.einsum('shr,str->sht', pick_rope, rope_block.astype(jnp.float32), precision=peak_score)) * score_scale
        live_token = jnp.arange(PAGE, dtype=jnp.int32)[None, None, :] < fill_block[:, None, None]
        slot_max = jnp.max(jnp.where(live_token, scores, NEG), axis=2)
        exponent = jnp.where(live_token, jnp.exp(scores - slot_max[:, :, None]), 0.0)
        slot_sum = jnp.sum(exponent, axis=2)
        weights = lax.optimization_barrier(exponent.astype(jnp.bfloat16)).astype(jnp.float32)
        slot_out = jnp.einsum('sht,stk->shk', weights, latent_f, precision=peak_score)
        owned = jnp.transpose(owner_block) > 0
        candidate = jnp.where(owned[:, :, None], slot_max[None, :, :], NEG)
        new_max = jnp.maximum(run_max, jnp.max(candidate, axis=1))
        carry_scale = jnp.exp(run_max - new_max)
        factor = jnp.where(owned[:, :, None], jnp.exp(candidate - new_max[:, None, :]), 0.0)
        run_sum = run_sum * carry_scale + jnp.einsum('bsh,sh->bh', factor, slot_sum, precision=peak_score)
        run_out = run_out * carry_scale[:, :, None] + jnp.einsum('bsh,shk->bhk', factor, slot_out, precision=peak_score)
        return (new_max, run_sum, run_out), None

    initial = (jnp.full((B, H), NEG, jnp.float32), jnp.zeros((B, H), jnp.float32), jnp.zeros((B, H, KVR), jnp.float32))
    final_state, unused = lax.scan(step_block, initial, (latent_blocks, rope_blocks, owner_blocks, fill_blocks))
    seq_max, seq_sum, seq_out = final_state
    attention_probs = (seq_out / seq_sum[:, :, None]).astype(jnp.bfloat16)
    value_rows = jnp.einsum('gre,req->grq', attention_probs.astype(jnp.float32), value_up_weight.astype(jnp.float32), precision=peak_score).astype(jnp.bfloat16)
    output = jnp.dot(value_rows.reshape(B, H * VDIM), w_out, preferred_element_type=jnp.float32).astype(jnp.bfloat16)
    return output
```

```python
import functools

import jax
import jax.numpy as jnp
from jax import lax
from jax.experimental import pallas as pl
from jax.experimental.pallas import tpu as pltpu
from jax.sharding import PartitionSpec as P

NEG = -1e30
MESH = pl.DeviceIdType.MESH
GROUP = 4
UNROLL = 2
QPARTS = 2
F32 = jnp.float32
BF16 = jnp.bfloat16


def make_plan(first_slot, page, lengths_ref, table_ref, plan_ref):
    seqs, pages = table_ref.shape
    slots_dev, wide = first_slot[1], plan_ref.shape[1]
    table = table_ref[...].astype(F32).T
    logical = lax.broadcasted_iota(jnp.int32, (pages, 1), 0)
    slot = lax.broadcasted_iota(jnp.int32, (pages, slots_dev), 1) + first_slot[0]
    slot = slot.astype(F32)
    fill = []
    for b in range(seqs):
        inside = jnp.clip(lengths_ref[b] - page * logical, 0, page)
        hit = table[:, b:b + 1] == slot
        fill.append(jnp.sum(jnp.where(hit, inside, 0), axis=0, keepdims=True))
    eye = (lax.broadcasted_iota(jnp.int32, (slots_dev, slots_dev), 0)
           == lax.broadcasted_iota(jnp.int32, (slots_dev, slots_dev), 1))
    earlier = (lax.broadcasted_iota(jnp.int32, (slots_dev, slots_dev), 1)
               < lax.broadcasted_iota(jnp.int32, (slots_dev, slots_dev), 0))
    at = lax.broadcasted_iota(jnp.int32, (1, wide), 1)
    start = jnp.zeros((1, 1), jnp.int32)
    owner = jnp.zeros((1, wide), jnp.int32)
    fresh = jnp.zeros((1, wide), jnp.int32)
    entry = jnp.zeros((1, wide), jnp.int32)
    target = jnp.full((slots_dev, 1), -1, jnp.int32)
    column = jnp.zeros((slots_dev, 1), jnp.int32)
    for b in range(seqs):
        owned = fill[b] > 0
        count = jnp.sum(owned.astype(jnp.int32), axis=1, keepdims=True)
        place = jnp.sum(jnp.where(earlier & owned, 1, 0), axis=1, keepdims=True)
        mine = jnp.sum(jnp.where(eye, fill[b], 0), axis=1, keepdims=True)
        target = jnp.where(mine > 0, start * GROUP + place, target)
        column = column + mine
        fresh = jnp.where(at == start, 1, fresh)
        start = start + (count + GROUP - 1) // GROUP
        owner = owner + (at >= start).astype(jnp.int32)
        entry = jnp.where((at == b) & (count > 0), start, entry)
    match = target == lax.broadcasted_iota(jnp.int32, (slots_dev, wide), 1)
    ids = lax.broadcasted_iota(jnp.int32, (slots_dev, wide), 0)
    plan_ref[0:1, :] = jnp.sum(jnp.where(match, ids, 0), axis=0, keepdims=True)
    plan_ref[1:2, :] = jnp.sum(jnp.where(match, column, 0), axis=0, keepdims=True)
    plan_ref[2:3, :] = jnp.minimum(owner, seqs - 1)
    plan_ref[3:4, :] = fresh
    plan_ref[4:5, :] = entry
    plan_ref[5:8, :] = jnp.zeros((3, wide), jnp.int32)


def merge(seqs, stats, parts):
    hs = stats[0].shape[0] // 2
    tops = [s[:hs] for s in stats]
    best = functools.reduce(jnp.maximum, tops)
    shares = [s[hs:] * jnp.exp(t - best) for s, t in zip(stats, tops)]
    total = functools.reduce(jnp.add, shares)
    inv = 1.0 / jnp.maximum(total, 1e-30)
    out = None
    for share, part in zip(shares, parts):
        share = share * inv
        column = jnp.concatenate([share[:, b:b + 1] for b in range(seqs)], axis=0)
        term = part * column
        out = term if out is None else out + term
    return out, best, total


def kernel(n, groups, pack, scale, nch,
           lengths_hbm, table_hbm, rope_hbm, qn_hbm, wuk_hbm, qr_hbm, lat_hbm, v_hbm, w_hbm, out_ref,
           lengths, table, rope, qn, wuk, qr, lat, w_buf, plan_v, plan, raw, flat, gath, q_all, turn,
           wide_rope, spread, run, tops, sums, ready, mix, st, ygot, yst, zout, zst, zgot, zgst, port,
           vbuf, vals, tx, rx,
           lsem, bulk, qs1, qr1, qs2, qr2, vs1, vr1, vs2, vr2, ys, yr, yss, ysr, zs, zr, zss, zsr, as_, ar, ms, mr):
    me = lax.axis_index("seq")
    half = lax.axis_index("mp")
    grp = lax.axis_index("groups")
    seqs, heads, _ = qn.shape
    cols = wuk.shape[1]
    slots, page, width = lat.shape
    hs = heads // n
    line = n // 2
    par = lax.rem(me, 2)
    row = me // 2
    partner = me + 1 - 2 * par
    share = groups == 2 and hs % 2 == 0
    hh = hs // 2 if share else hs
    voff = grp * hh if share else 0
    hp = heads // QPARTS

    barrier = pltpu.get_barrier_semaphore()
    for k in range(1, n):
        pl.semaphore_signal(barrier, inc=1, device_id={"seq": lax.rem(me + k, n)}, device_id_type=MESH)
    pl.semaphore_signal(barrier, inc=1, device_id={"mp": 1 - half}, device_id_type=MESH)
    if share:
        pl.semaphore_signal(barrier, inc=1, device_id={"groups": 1 - grp}, device_id_type=MESH)

    loads = [pltpu.make_async_copy(a, b, lsem.at[i]) for i, (a, b) in enumerate((
        (qn_hbm, qn), (wuk_hbm, wuk), (lengths_hbm, lengths), (table_hbm, table), (qr_hbm, qr), (rope_hbm, rope)))]
    for copy in loads:
        copy.start()
    nb = bulk.shape[0] // 2
    step_l = slots // nb
    big = [pltpu.make_async_copy(lat_hbm.at[pl.ds(i * step_l, step_l)], lat.at[pl.ds(i * step_l, step_l)], bulk.at[i])
           for i in range(nb)]
    step_w = w_buf.shape[0] // nb
    bigw = [pltpu.make_async_copy(w_hbm.at[pl.ds(i * step_w, step_w)], w_buf.at[pl.ds(i * step_w, step_w)], bulk.at[nb + i])
            for i in range(nb)]
    own_v = pltpu.make_async_copy(v_hbm.at[pl.ds(me * hs, hs)], vbuf.at[me], lsem.at[6])

    def remote(src, dst, s, r, where):
        return pltpu.make_async_remote_copy(
            src_ref=src, dst_ref=dst, send_sem=s, recv_sem=r, device_id=where, device_id_type=MESH)

    loads[0].wait()
    for b in range(seqs):
        flat[b * heads:(b + 1) * heads, :] = qn[b].astype(F32)
    loads[1].wait()
    for copy in big:
        copy.start()

    def q_copy(block, i, k, peer, s, r):
        return remote(gath.at[block, i], gath.at[block, i], s.at[i * line + k], r.at[i * line + k], {"seq": peer})

    along, across = [], []
    for i in range(QPARTS):
        for h in range(i * hp, (i + 1) * hp):
            q = flat[pl.ds(h, seqs, stride=heads), :].astype(BF16)
            raw[h * seqs:(h + 1) * seqs, :] = lax.dot_general(
                q, wuk[h], (((1,), (1,)), ((), ())), preferred_element_type=F32)
        for p in range(seqs // pack):
            parts = [raw[pl.ds(i * hp * seqs + p * pack + j, hp, stride=seqs), :] for j in range(pack)]
            whole = parts[0] if pack == 1 else jnp.concatenate(parts, axis=1)
            gath[me, i, p * hp:(p + 1) * hp, :] = whole.astype(BF16)
        if i == 0:
            pl.semaphore_wait(barrier, n - 1 + 1 + int(share))
        for k in range(1, line):
            copy = q_copy(me, i, k, lax.rem(me + 2 * k, n), qs1, qr1)
            copy.start()
            along.append((i, k, copy))
        copy = q_copy(me, i, 0, partner, qs2, qr2)
        copy.start()
        across.append(copy)

    loads[2].wait()
    loads[3].wait()
    make_plan((me * slots, slots), page, lengths, table, plan_v)
    plan_copy = pltpu.make_async_copy(plan_v, plan, lsem.at[7])
    plan_copy.start()
    loads[4].wait()
    loads[5].wait()
    own_v.start()
    per = page * 128 // rope.shape[1]
    lane = lax.broadcasted_iota(jnp.int32, (slots, 128), 1) // (128 // per)

    def widen(i):
        x = rope[:, i * 128:(i + 1) * 128].astype(F32)
        for j in range(per):
            wide_rope[pl.ds(i * per + j, slots, stride=page), :] = jnp.where(lane == j, x, 0.0)

    fillers = list(range(rope.shape[1] // 128))
    each = -(-len(fillers) // max(1, len(along)))
    for i, k, copy in along:
        for f in fillers[:each]:
            widen(f)
        fillers = fillers[each:]
        copy.wait_recv()
        forward = q_copy(lax.rem(me - 2 * k + n, n), i, k, partner, qs2, qr2)
        forward.start()
        across.append(forward)

    def v_copy(k):
        peer = lax.rem(me + k, n)
        return remote(v_hbm.at[pl.ds(peer * hs + voff, hh)], vbuf.at[me, pl.ds(voff, hh)], vs1.at[k], vr1.at[k],
                      {"seq": peer})

    def twin_copy(k):
        s = lax.rem(me - k + n, n)
        return remote(vbuf.at[s, pl.ds(voff, hh)], vbuf.at[s, pl.ds(voff, hh)], vs2.at[k], vr2.at[k],
                      {"groups": 1 - grp})

    for k in range(2, n, 2):
        v_copy(k).start()

    def narrow(i, _):
        spread[i] = wide_rope[pl.ds(pl.multiple_of(i * page, page), page), :].astype(BF16)
        return 0

    lax.fori_loop(0, slots, narrow, 0, unroll=4)
    for b in range(seqs):
        turn[b] = jnp.concatenate([qr[b]] * (128 // qr.shape[2]), axis=1)
    run[0] = jnp.zeros(run.shape[1:], F32)
    tops[0] = jnp.full(tops.shape[1:], NEG, F32)
    sums[0] = jnp.zeros(sums.shape[1:], F32)
    plan_copy.wait()
    for copy in big:
        copy.wait()
    for copy in bigw:
        copy.start()
    for i, k, copy in along:
        copy.wait_send()
    for copy in across:
        copy.wait()
    for k in range(1, n, 2):
        v_copy(k).start()
    for i in range(QPARTS):
        for s in range(n):
            for b in range(seqs):
                at = b % pack * cols
                q_all[b, i * hp:(i + 1) * hp, s * cols:(s + 1) * cols] = gath[
                    s, i, b // pack * hp:(b // pack + 1) * hp, at:at + cols]

    tokens = GROUP * page
    tlane = lax.broadcasted_iota(jnp.int32, (1, tokens), 1)
    nt = (((1,), (1,)), ((), ()))

    def keys_of(c):
        return jnp.concatenate([lat[plan[0, c * GROUP + g]] for g in range(GROUP)], axis=0)

    def score_of(c):
        b = plan[2, c]
        turned = jnp.concatenate([spread[plan[0, c * GROUP + g]] for g in range(GROUP)], axis=0)
        limit = jnp.zeros((1, tokens), jnp.int32)
        for g in range(GROUP):
            limit = jnp.where(tlane // page == g, plan[1, c * GROUP + g] + g * page, limit)
        score = lax.dot_general(turn[b], turned, nt, preferred_element_type=F32)
        score = (score + lax.dot_general(q_all[b], keys_of(c), nt, preferred_element_type=F32)) * scale
        return jnp.where(tlane < limit, score, NEG)

    for u in range(UNROLL):
        ready[u] = score_of(u)

    def step(it, _):
        first = it * UNROLL
        scores = [ready[u] for u in range(UNROLL)]
        upcoming = [score_of(first + UNROLL + u) for u in range(UNROLL)]
        top, total, acc = tops[first][:, :1], sums[first][:, :1], run[first]
        for u in range(UNROLL):
            c = first + u
            old = jnp.where(plan[3, c] > 0, NEG, top)
            top = jnp.maximum(old, jnp.max(scores[u], axis=1, keepdims=True))
            weight = jnp.exp(scores[u] - top)
            carry = jnp.exp(old - top)
            product = jnp.dot(weight.astype(BF16), keys_of(c), preferred_element_type=F32)
            total = total * carry + jnp.sum(weight, axis=1, keepdims=True)
            acc = acc * carry + product
            tops[c + 1] = jnp.broadcast_to(top, tops.shape[1:])
            sums[c + 1] = jnp.broadcast_to(total, sums.shape[1:])
            run[c + 1] = acc
        for u in range(UNROLL):
            ready[u] = upcoming[u]
        return 0

    trips = nch // UNROLL
    relays = list(range(2, n, 2)) if share else []
    done = 0
    if relays:
        lead = trips - trips // 5 * len(relays)
        stride = trips // 5
        lax.fori_loop(0, lead, step, 0)

        def segment(j, _):
            v_copy(2 * j + 2).wait_recv()
            twin_copy(2 * j + 2).start()
            lax.fori_loop(lead + j * stride, lead + (j + 1) * stride, step, 0)
            return 0

        lax.fori_loop(0, len(relays), segment, 0)
    else:
        lax.fori_loop(0, trips, step, 0)

    ids = lax.broadcasted_iota(jnp.int32, (heads, 128), 1)
    all_top = jnp.full((heads, 128), NEG, F32)
    all_sum = jnp.zeros((heads, 128), F32)
    for p in range(seqs // 2):
        pair = []
        for b in (2 * p, 2 * p + 1):
            entry = plan[4, b]
            bt, bs = tops[entry], sums[entry]
            all_top = jnp.where(ids == b, bt, all_top)
            all_sum = jnp.where(ids == b, bs, all_sum)
            pair.append(run[entry] * (1.0 / jnp.maximum(bs[:, :1], 1e-30)))
        for d in range(n):
            mix[d, 2 * p * hs:2 * (p + 1) * hs, :] = jnp.concatenate(
                [x[d * hs:(d + 1) * hs] for x in pair], axis=0).astype(BF16)
    for d in range(n):
        st[d, :hs, :] = all_top[d * hs:(d + 1) * hs]
        st[d, hs:, :] = all_sum[d * hs:(d + 1) * hs]

    order = list(range(1, line)) + [0]
    sent = []
    for k in order:
        r = lax.rem(row + k, line)
        d = 2 * r + 1 - par
        for src, dst, s, rr in ((st, yst, yss, ysr), (mix, ygot, ys, yr)):
            copy = remote(src.at[d], dst.at[r], s.at[k], rr.at[k], {"seq": partner})
            copy.start()
            sent.append(copy)
    if share:
        for k in (1, 3):
            v_copy(k).wait_recv()
            twin_copy(k).start()
    onward = []
    for i, k in enumerate(order):
        sent[2 * i].wait_recv()
        sent[2 * i + 1].wait_recv()
        r = lax.rem(row + k, line)
        mine = 2 * r + par
        o, best, total = merge(seqs, [st[mine], yst[r]], [mix[mine].astype(F32), ygot[r].astype(F32)])
        zst[k, :hs, :] = best
        zst[k, hs:, :] = total
        zout[k] = o.astype(BF16)
        if k:
            for src, dst, s, rr in ((zst, zgst, zss, zsr), (zout, zgot, zs, zr)):
                copy = remote(src.at[k], dst.at[k], s.at[k], rr.at[k], {"seq": lax.rem(me + 2 * k, n)})
                copy.start()
                onward.append(copy)
    if share:
        for k in range(5, n, 2):
            v_copy(k).wait_recv()
            twin_copy(k).start()
    for copy in onward:
        copy.wait_recv()
    o, _, _ = merge(seqs, [zst[0]] + [zgst[k] for k in range(1, line)],
                    [zout[0].astype(F32)] + [zgot[k].astype(F32) for k in range(1, line)])
    blocks = width // 128
    for j in range(blocks):
        port[j] = o[:, j * 128:(j + 1) * 128]

    own_v.wait()
    for k in range(1, n):
        if share:
            twin_copy(k).wait_recv()
        else:
            v_copy(k).wait_recv()
    vdim = vbuf.shape[3]
    for h in range(hs):
        x = jnp.concatenate([port[j, pl.ds(h, seqs, stride=hs), :] for j in range(blocks)], axis=1).astype(BF16)
        wv = vbuf[:, h].reshape(width, vdim)
        vals[me, :, h * vdim:(h + 1) * vdim] = jnp.dot(x, wv, preferred_element_type=F32).astype(BF16)
    copies = []
    for k in range(1, n):
        copy = remote(vals.at[me], vals.at[me], as_.at[k], ar.at[k], {"seq": lax.rem(me + k, n)})
        copy.start()
        copies.append(copy)
    for copy in bigw:
        copy.wait()
    rows = hs * vdim
    res = None
    for k in range(n):
        src = lax.rem(me - k + n, n)
        if k:
            copies[k - 1].wait_recv()
        at = pl.ds(pl.multiple_of(src * rows, rows), rows)
        product = jnp.dot(vals[src], w_buf[at, :], preferred_element_type=F32)
        res = product if res is None else res + product
    wide = res.shape[1] // 2
    low, high = res[:, :wide], res[:, wide:]
    first = half == 0
    tx[...] = jnp.where(first, high, low)
    copy = remote(tx, rx, ms, mr, {"mp": 1 - half})
    copy.start()
    for c in copies + sent + onward:
        c.wait_send()
    for k in range(1, n):
        v_copy(k).wait_send()
        if share:
            twin_copy(k).wait_send()
    copy.wait()
    out_ref[...] = (jnp.where(first, low, high) + rx[...]).astype(BF16)


def local(n, groups, latent_cache, rope_cache, q_nope, q_rope, w_uk, value_up_weight, w_out, page_table, lengths):
    slots, page, width = latent_cache.shape
    seqs, heads, nope = q_nope.shape
    rope_w = q_rope.shape[2]
    cols = w_uk.shape[2]
    vdim = value_up_weight.shape[2]
    scale = (nope + rope_w) ** (-0.5)
    pack = max(1, min(seqs, 128 // cols))
    lanes = pack * cols
    hs = heads // n
    line = n // 2
    rows = seqs * hs
    wide = w_out.shape[1]
    nch = (slots + seqs * (GROUP - 1)) // GROUP
    nch = -(-nch // UNROLL) * UNROLL
    pw = ((nch + UNROLL) * GROUP + 127) // 128 * 128
    vm = pl.BlockSpec(memory_space=pltpu.VMEM)
    hbm = pl.BlockSpec(memory_space=pl.ANY)
    dma = pltpu.SemaphoreType.DMA
    vmem = pltpu.VMEM
    bulk = 8
    return pl.pallas_call(
        functools.partial(kernel, n, groups, pack, scale, nch),
        out_shape=jax.ShapeDtypeStruct((seqs, wide // 2), BF16),
        in_specs=[hbm] * 9, out_specs=vm,
        scratch_shapes=[
            pltpu.SMEM(lengths.shape, jnp.int32),
            vmem(page_table.shape, jnp.int32),
            vmem(rope_cache.shape, BF16),
            vmem(q_nope.shape, BF16),
            vmem((heads, cols, nope), BF16),
            vmem(q_rope.shape, BF16),
            vmem(latent_cache.shape, BF16),
            vmem(w_out.shape, BF16),
            vmem((8, pw), jnp.int32),
            pltpu.SMEM((8, pw), jnp.int32),
            vmem((heads * seqs, cols), F32),
            vmem((heads * seqs, nope), F32),
            vmem((n, QPARTS, seqs // pack * heads // QPARTS, lanes), BF16),
            vmem((seqs, heads, width), BF16),
            vmem((seqs, heads, 128), BF16),
            vmem((slots * page, 128), F32),
            vmem((slots, page, 128), BF16),
            vmem((nch + 1, heads, width), F32),
            vmem((nch + 1, heads, 128), F32),
            vmem((nch + 1, heads, 128), F32),
            vmem((UNROLL, heads, GROUP * page), F32),
            vmem((n, rows, width), BF16),
            vmem((n, 2 * hs, 128), F32),
            vmem((line, rows, width), BF16),
            vmem((line, 2 * hs, 128), F32),
            vmem((line, rows, width), BF16),
            vmem((line, 2 * hs, 128), F32),
            vmem((line, rows, width), BF16),
            vmem((line, 2 * hs, 128), F32),
            vmem((width // 128, rows, 128), F32),
            vmem((n, hs, cols, vdim), BF16),
            vmem((n, seqs, hs * vdim), BF16),
            vmem((seqs, wide // 2), F32),
            vmem((seqs, wide // 2), F32),
            dma((8,)), dma((2 * bulk,)),
            dma((QPARTS * line,)), dma((QPARTS * line,)), dma((QPARTS * line,)), dma((QPARTS * line,)),
            dma((n,)), dma((n,)), dma((n,)), dma((n,)),
            dma((line,)), dma((line,)), dma((line,)), dma((line,)),
            dma((line,)), dma((line,)), dma((line,)), dma((line,)),
            dma((n,)), dma((n,)), dma, dma,
        ],
        compiler_params=pltpu.CompilerParams(
            has_side_effects=True, collective_id=1, vmem_limit_bytes=60 * 1024 * 1024),
        name="decode",
    )(lengths, page_table, rope_cache, q_nope, w_uk.transpose(0, 2, 1), q_rope, latent_cache, value_up_weight, w_out)


def solution(mesh):
    return jax.shard_map(
        functools.partial(local, mesh.shape["seq"], mesh.shape["groups"]),
        mesh=mesh,
        in_specs=(
            P(("groups", "seq"), None, None),
            P(("groups", "seq"), None),
            P("groups", "mp", None),
            P("groups", "mp", None),
            P("mp", None, "seq"),
            P("mp", "seq", None),
            P("mp", "seq"),
            P("groups", None),
            P("groups"),
        ),
        out_specs=P("groups", ("seq", "mp")),
        check_vma=False,
    )
```

```python
import functools
import math

import jax
import jax.numpy as jnp
from jax import lax
from jax.experimental import pallas as pl
from jax.experimental.pallas import tpu as pltpu
from jax.sharding import PartitionSpec as P

NEG = -1e30
MESH = pl.DeviceIdType.MESH
GROUP = 4
UNROLL = 10
QPARTS = 2
F32 = jnp.float32
BF16 = jnp.bfloat16


def make_plan(first_slot, page, lengths_ref, table_ref, plan_ref):
    seqs, pages = table_ref.shape
    slots_dev, wide = first_slot[1], plan_ref.shape[1]
    table = table_ref[...].astype(F32).T
    logical = lax.broadcasted_iota(jnp.int32, (pages, 1), 0)
    slot = lax.broadcasted_iota(jnp.int32, (pages, slots_dev), 1) + first_slot[0]
    slot = slot.astype(F32)
    fill = []
    for b in range(seqs):
        inside = jnp.clip(lengths_ref[b] - page * logical, 0, page)
        hit = table[:, b:b + 1] == slot
        fill.append(jnp.sum(jnp.where(hit, inside, 0), axis=0, keepdims=True))
    eye = (lax.broadcasted_iota(jnp.int32, (slots_dev, slots_dev), 0)
           == lax.broadcasted_iota(jnp.int32, (slots_dev, slots_dev), 1))
    earlier = (lax.broadcasted_iota(jnp.int32, (slots_dev, slots_dev), 1)
               < lax.broadcasted_iota(jnp.int32, (slots_dev, slots_dev), 0))
    at = lax.broadcasted_iota(jnp.int32, (1, wide), 1)
    start = jnp.zeros((1, 1), jnp.int32)
    owner = jnp.zeros((1, wide), jnp.int32)
    fresh = jnp.zeros((1, wide), jnp.int32)
    entry = jnp.zeros((1, wide), jnp.int32)
    target = jnp.full((slots_dev, 1), -1, jnp.int32)
    column = jnp.zeros((slots_dev, 1), jnp.int32)
    for b in range(seqs):
        owned = fill[b] > 0
        count = jnp.sum(owned.astype(jnp.int32), axis=1, keepdims=True)
        place = jnp.sum(jnp.where(earlier & owned, 1, 0), axis=1, keepdims=True)
        mine = jnp.sum(jnp.where(eye, fill[b], 0), axis=1, keepdims=True)
        target = jnp.where(mine > 0, start * GROUP + place, target)
        column = column + mine
        fresh = jnp.where(at == start, 1, fresh)
        start = start + (count + GROUP - 1) // GROUP
        owner = owner + (at >= start).astype(jnp.int32)
        entry = jnp.where((at == b) & (count > 0), start, entry)
    match = target == lax.broadcasted_iota(jnp.int32, (slots_dev, wide), 1)
    ids = lax.broadcasted_iota(jnp.int32, (slots_dev, wide), 0)
    plan_ref[0:1, :] = jnp.sum(jnp.where(match, ids, 0), axis=0, keepdims=True)
    plan_ref[1:2, :] = jnp.sum(jnp.where(match, column, 0), axis=0, keepdims=True)
    plan_ref[2:3, :] = jnp.minimum(owner, seqs - 1)
    plan_ref[3:4, :] = fresh
    plan_ref[4:5, :] = entry
    plan_ref[5:8, :] = jnp.zeros((3, wide), jnp.int32)


def merge(seqs, stats, parts):
    hs = stats[0].shape[0] // 2
    tops = [s[:hs] for s in stats]
    best = functools.reduce(jnp.maximum, tops)
    shares = [s[hs:] * jnp.exp2(t - best) for s, t in zip(stats, tops)]
    total = functools.reduce(jnp.add, shares)
    inv = 1.0 / jnp.maximum(total, 1e-30)
    out = None
    for share, part in zip(shares, parts):
        share = share * inv
        column = jnp.concatenate([share[:, b:b + 1] for b in range(seqs)], axis=0)
        term = part * column
        out = term if out is None else out + term
    return out, best, total


def kernel(n, groups, pack, scale, nch,
           lengths_hbm, table_hbm, rope_hbm, qn_hbm, wuk_hbm, qr_hbm, lat_hbm, v_hbm, w_hbm, out_ref,
           lengths, table, rope, qn, wuk, qr, lat, w_buf, plan_v, plan, raw, flat, gath, q_near, q_far, turn,
           wide_rope, spread, run, tops, sums, peak, part, mix, st, ygot, yst, zout, zst, zgot, zgst, port,
           vbuf, vals, tx, rx,
           lsem, bulk, qs1, qr1, qs2, qr2, vs1, vr1, vs2, vr2, ys, yr, yss, ysr, zs, zr, zss, zsr, as_, ar, ms, mr):
    me = lax.axis_index("seq")
    half = lax.axis_index("mp")
    grp = lax.axis_index("groups")
    seqs, heads, _ = qn.shape
    cols = wuk.shape[1]
    _, slots, page, wing = lat.shape
    width = 2 * wing
    hs = heads // n
    line = n // 2
    par = lax.rem(me, 2)
    row = me // 2
    partner = me + 1 - 2 * par
    share = groups == 2 and hs % 2 == 0
    hh = hs // 2 if share else hs
    voff = grp * hh if share else 0
    hp = heads // QPARTS
    near_n = line // 2
    side, pos = row // near_n, lax.rem(row, near_n)

    def along_of(j, sign):
        other, k = (0, j) if j < near_n else (1, j - near_n)
        at = lax.rem(pos + sign * k + near_n, near_n)
        return 2 * ((side + other * (1 - 2 * side)) * near_n + at) + par

    barrier = pltpu.get_barrier_semaphore()
    for k in range(1, n):
        pl.semaphore_signal(barrier, inc=1, device_id={"seq": lax.rem(me + k, n)}, device_id_type=MESH)
    pl.semaphore_signal(barrier, inc=1, device_id={"mp": 1 - half}, device_id_type=MESH)
    if share:
        pl.semaphore_signal(barrier, inc=1, device_id={"groups": 1 - grp}, device_id_type=MESH)

    loads = [pltpu.make_async_copy(a, b, lsem.at[i]) for i, (a, b) in enumerate((
        (qn_hbm, qn), (wuk_hbm, wuk), (lengths_hbm, lengths), (table_hbm, table), (qr_hbm, qr), (rope_hbm, rope)))]
    for copy in loads:
        copy.start()
    nb = bulk.shape[0] // 2
    step_l = 2 * slots // nb
    big = [pltpu.make_async_copy(
        lat_hbm.at[pl.ds(i // 2 * step_l, step_l), :, pl.ds(i % 2 * wing, wing)],
        lat.at[i % 2, pl.ds(i // 2 * step_l, step_l)], bulk.at[i]) for i in range(nb)]
    step_w = w_buf.shape[0] // nb
    bigw = [pltpu.make_async_copy(w_hbm.at[pl.ds(i * step_w, step_w)], w_buf.at[pl.ds(i * step_w, step_w)], bulk.at[nb + i])
            for i in range(nb)]
    own_v = pltpu.make_async_copy(v_hbm.at[pl.ds(me * hs, hs)], vbuf.at[me], lsem.at[6])

    def remote(src, dst, s, r, where):
        return pltpu.make_async_remote_copy(
            src_ref=src, dst_ref=dst, send_sem=s, recv_sem=r, device_id=where, device_id_type=MESH)

    loads[0].wait()
    for b in range(seqs):
        flat[b * heads:(b + 1) * heads, :] = qn[b].astype(F32)
    loads[1].wait()
    for copy in big:
        copy.start()

    def q_copy(block, i, k, peer, s, r):
        return remote(gath.at[block, i], gath.at[block, i], s.at[i * line + k], r.at[i * line + k], {"seq": peer})

    along, across = [], []
    for i in range(QPARTS):
        for h in range(i * hp, (i + 1) * hp):
            q = flat[pl.ds(h, seqs, stride=heads), :].astype(BF16)
            raw[h * seqs:(h + 1) * seqs, :] = lax.dot_general(
                q, wuk[h], (((1,), (1,)), ((), ())), preferred_element_type=F32)
        for p in range(seqs // pack):
            parts = [raw[pl.ds(i * hp * seqs + p * pack + j, hp, stride=seqs), :] for j in range(pack)]
            whole = parts[0] if pack == 1 else jnp.concatenate(parts, axis=1)
            gath[me, i, p * hp:(p + 1) * hp, :] = whole.astype(BF16)
        if i == 0:
            pl.semaphore_wait(barrier, n - 1 + 1 + int(share))
        for k in range(1, line):
            copy = q_copy(me, i, k, along_of(k, 1), qs1, qr1)
            copy.start()
            along.append((i, k, copy))
        copy = q_copy(me, i, 0, partner, qs2, qr2)
        copy.start()
        across.append((0, copy))

    def v_copy(k):
        peer = lax.rem(me + k, n)
        return remote(v_hbm.at[pl.ds(peer * hs + voff, hh)], vbuf.at[me, pl.ds(voff, hh)], vs1.at[k], vr1.at[k],
                      {"seq": peer})

    def twin_copy(k):
        s = lax.rem(me - k + n, n)
        return remote(vbuf.at[s, pl.ds(voff, hh)], vbuf.at[s, pl.ds(voff, hh)], vs2.at[k], vr2.at[k],
                      {"groups": 1 - grp})

    loads[2].wait()
    loads[3].wait()
    make_plan((me * slots, slots), page, lengths, table, plan_v)
    plan_copy = pltpu.make_async_copy(plan_v, plan, lsem.at[7])
    plan_copy.start()
    loads[4].wait()
    loads[5].wait()
    own_v.start()
    per = page * 128 // rope.shape[1]
    pitch = wide_rope.shape[0] // slots
    lane = lax.broadcasted_iota(jnp.int32, (slots, 128), 1) // (128 // per)

    def widen(i):
        x = rope[:, i * 128:(i + 1) * 128].astype(F32)
        for j in range(per):
            wide_rope[pl.ds(i * per + j, slots, stride=pitch), :] = jnp.where(lane == j, x, 0.0)

    def narrow(i, _):
        spread[i] = wide_rope[pl.ds(pl.multiple_of(i * pitch, 8), page), :].astype(BF16)
        return 0

    along.sort(key=lambda x: (x[1] >= near_n, x[0], x[1]))
    steps = rope.shape[1] // 128
    share_w = -(-steps // max(1, len(along) // 2))
    for i, (q, k, copy) in enumerate(along):
        for f in range(min(steps, i * share_w), min(steps, (i + 1) * share_w)):
            widen(f)
        if (i + 1) * share_w >= steps > i * share_w:
            lax.fori_loop(0, slots, narrow, 0, unroll=4)
        copy.wait_recv()
        forward = q_copy(along_of(k, -1), q, k, partner, qs2, qr2)
        forward.start()
        across.append((k, forward))

    for k in range(2, n, 2):
        v_copy(k).start()
    for k in range(1, n, 2):
        v_copy(k).start()

    for b in range(seqs):
        turn[b] = jnp.concatenate([qr[b]] * (128 // qr.shape[2]), axis=1)
    run[0] = jnp.zeros(run.shape[1:], F32)
    tops[0] = jnp.full(tops.shape[1:], NEG, F32)
    sums[0] = jnp.zeros(sums.shape[1:], F32)
    plan_copy.wait()
    for copy in big:
        copy.wait()
    for copy in bigw:
        copy.start()

    def assemble(first, dst):
        for i in range(QPARTS):
            for s in range(n // 2):
                for b in range(seqs):
                    at = b % pack * cols
                    dst[b, i * hp:(i + 1) * hp, s * cols:(s + 1) * cols] = gath[
                        first + s, i, b // pack * hp:(b // pack + 1) * hp, at:at + cols]

    tokens = GROUP * page
    tlane = lax.broadcasted_iota(jnp.int32, (1, tokens), 1)
    nt = (((1,), (1,)), ((), ()))

    def slots_of(ref, c):
        return jnp.concatenate([ref[plan[0, c * GROUP + g]] for g in range(GROUP)], axis=0)

    def first_pass(it, _):
        for u in range(UNROLL):
            c = it * UNROLL + u
            b = plan[2, c]
            limit = jnp.zeros((1, tokens), jnp.int32)
            for g in range(GROUP):
                limit = jnp.where(tlane // page == g, plan[1, c * GROUP + g] + g * page, limit)
            score = lax.dot_general(turn[b], slots_of(spread, c), nt, preferred_element_type=F32)
            score = score + lax.dot_general(q_near[b], slots_of(lat.at[side], c), nt, preferred_element_type=F32)
            part[c] = jnp.where(tlane < limit, score, NEG)
        return 0

    for k, copy in across:
        if k < near_n:
            copy.wait_recv()
    assemble(side * (n // 2), q_near)
    trips = nch // UNROLL
    lax.fori_loop(0, trips, first_pass, 0)
    for k, copy in across:
        if k >= near_n:
            copy.wait_recv()
    assemble((1 - side) * (n // 2), q_far)

    def second_pass(it, _):
        top = tops[it * UNROLL]
        for u in range(UNROLL):
            c = it * UNROLL + u
            far = lax.dot_general(q_far[plan[2, c]], slots_of(lat.at[1 - side], c), nt, preferred_element_type=F32)
            score = (part[c] + far) * scale
            part[c] = score
            top = jnp.where(plan[3, c] > 0, NEG, top)
            for j in range(tokens // 128):
                top = jnp.maximum(top, score[:, j * 128:(j + 1) * 128])
            tops[c + 1] = top
        return 0

    lax.fori_loop(0, trips, second_pass, 0)
    for b in range(seqs):
        peak[b] = jnp.broadcast_to(jnp.max(tops[plan[4, b]], axis=1, keepdims=True), peak.shape[1:])

    def third_pass(it, _):
        acc, total = run[it * UNROLL], sums[it * UNROLL]
        for u in range(UNROLL):
            c = it * UNROLL + u
            top = peak[plan[2, c]]
            keep = jnp.where(plan[3, c] > 0, 0.0, 1.0)
            weight = [jnp.exp2(part[c, :, j * 128:(j + 1) * 128] - top) for j in range(tokens // 128)]
            total = total * keep + functools.reduce(jnp.add, weight)
            weight = jnp.concatenate([x.astype(BF16) for x in weight], axis=1)
            product = jnp.concatenate(
                [jnp.dot(weight, slots_of(lat.at[j], c), preferred_element_type=F32) for j in range(2)], axis=1)
            acc = acc * keep + product
            sums[c + 1] = total
            run[c + 1] = acc
        return 0

    lax.fori_loop(0, trips, third_pass, 0)

    if share:
        for k in range(2, n, 2):
            v_copy(k).wait_recv()
            twin_copy(k).start()
    ids = lax.broadcasted_iota(jnp.int32, (heads, 128), 1)
    all_top = jnp.full((heads, 128), NEG, F32)
    all_sum = jnp.zeros((heads, 128), F32)
    for p in range(seqs // 2):
        pair = []
        for b in (2 * p, 2 * p + 1):
            entry = plan[4, b]
            total = jnp.sum(sums[entry], axis=1, keepdims=True)
            all_top = jnp.where(ids == b, peak[b], all_top)
            all_sum = jnp.where(ids == b, total, all_sum)
            pair.append(run[entry] * (1.0 / jnp.maximum(total, 1e-30)))
        for d in range(n):
            mix[d, 2 * p * hs:2 * (p + 1) * hs, :] = jnp.concatenate(
                [x[d * hs:(d + 1) * hs] for x in pair], axis=0).astype(BF16)
    for d in range(n):
        st[d, :hs, :] = all_top[d * hs:(d + 1) * hs]
        st[d, hs:, :] = all_sum[d * hs:(d + 1) * hs]

    order = list(range(1, line)) + [0]
    sent = []
    for k in order:
        r = lax.rem(row + k, line)
        d = 2 * r + 1 - par
        for src, dst, s, rr in ((st, yst, yss, ysr), (mix, ygot, ys, yr)):
            copy = remote(src.at[d], dst.at[r], s.at[k], rr.at[k], {"seq": partner})
            copy.start()
            sent.append(copy)
    if share:
        for k in (1, 3):
            v_copy(k).wait_recv()
            twin_copy(k).start()
    onward = []
    for i, k in enumerate(order):
        sent[2 * i].wait_recv()
        sent[2 * i + 1].wait_recv()
        r = lax.rem(row + k, line)
        mine = 2 * r + par
        o, best, total = merge(seqs, [st[mine], yst[r]], [mix[mine].astype(F32), ygot[r].astype(F32)])
        zst[k, :hs, :] = best
        zst[k, hs:, :] = total
        zout[k] = o.astype(BF16)
        if k:
            for src, dst, s, rr in ((zst, zgst, zss, zsr), (zout, zgot, zs, zr)):
                copy = remote(src.at[k], dst.at[k], s.at[k], rr.at[k], {"seq": lax.rem(me + 2 * k, n)})
                copy.start()
                onward.append(copy)
    if share:
        for k in range(5, n, 2):
            v_copy(k).wait_recv()
            twin_copy(k).start()
    for copy in onward:
        copy.wait_recv()
    o, _, _ = merge(seqs, [zst[0]] + [zgst[k] for k in range(1, line)],
                    [zout[0].astype(F32)] + [zgot[k].astype(F32) for k in range(1, line)])
    blocks = width // 128
    for j in range(blocks):
        port[j] = o[:, j * 128:(j + 1) * 128]

    own_v.wait()
    for k in range(1, n):
        if share:
            twin_copy(k).wait_recv()
        else:
            v_copy(k).wait_recv()
    vdim = vbuf.shape[3]
    for h in range(hs):
        x = jnp.concatenate([port[j, pl.ds(h, seqs, stride=hs), :] for j in range(blocks)], axis=1).astype(BF16)
        wv = vbuf[:, h].reshape(width, vdim)
        vals[me, :, h * vdim:(h + 1) * vdim] = jnp.dot(x, wv, preferred_element_type=F32).astype(BF16)
    copies = []
    for k in range(1, n):
        copy = remote(vals.at[me], vals.at[me], as_.at[k], ar.at[k], {"seq": lax.rem(me + k, n)})
        copy.start()
        copies.append(copy)
    for copy in bigw:
        copy.wait()
    rows = hs * vdim
    res = None
    for k in range(n):
        src = lax.rem(me - k + n, n)
        if k:
            copies[k - 1].wait_recv()
        at = pl.ds(pl.multiple_of(src * rows, rows), rows)
        product = jnp.dot(vals[src], w_buf[at, :], preferred_element_type=F32)
        res = product if res is None else res + product
    wide = res.shape[1] // 2
    low, high = res[:, :wide], res[:, wide:]
    first = half == 0
    tx[...] = jnp.where(first, high, low)
    copy = remote(tx, rx, ms, mr, {"mp": 1 - half})
    copy.start()
    for c in copies + sent + onward + [x[2] for x in along] + [x[1] for x in across]:
        c.wait_send()
    for k in range(1, n):
        v_copy(k).wait_send()
        if share:
            twin_copy(k).wait_send()
    copy.wait()
    out_ref[...] = (jnp.where(first, low, high) + rx[...]).astype(BF16)


def local(n, groups, latent_cache, rope_cache, q_nope, q_rope, w_uk, value_up_weight, w_out, page_table, lengths):
    slots, page, width = latent_cache.shape
    seqs, heads, nope = q_nope.shape
    rope_w = q_rope.shape[2]
    cols = w_uk.shape[2]
    vdim = value_up_weight.shape[2]
    scale = (nope + rope_w) ** (-0.5) * math.log2(math.e)
    pack = max(1, min(seqs, 128 // cols))
    lanes = pack * cols
    hs = heads // n
    line = n // 2
    rows = seqs * hs
    wide = w_out.shape[1]
    nch = (slots + seqs * (GROUP - 1)) // GROUP
    nch = -(-nch // UNROLL) * UNROLL
    pw = (nch * GROUP + 127) // 128 * 128
    vm = pl.BlockSpec(memory_space=pltpu.VMEM)
    hbm = pl.BlockSpec(memory_space=pl.ANY)
    dma = pltpu.SemaphoreType.DMA
    vmem = pltpu.VMEM
    bulk = 8
    return pl.pallas_call(
        functools.partial(kernel, n, groups, pack, scale, nch),
        out_shape=jax.ShapeDtypeStruct((seqs, wide // 2), BF16),
        in_specs=[hbm] * 9, out_specs=vm,
        scratch_shapes=[
            pltpu.SMEM(lengths.shape, jnp.int32),
            vmem(page_table.shape, jnp.int32),
            vmem(rope_cache.shape, BF16),
            vmem(q_nope.shape, BF16),
            vmem((heads, cols, nope), BF16),
            vmem(q_rope.shape, BF16),
            vmem((2, slots, page, width // 2), BF16),
            vmem(w_out.shape, BF16),
            vmem((8, pw), jnp.int32),
            pltpu.SMEM((8, pw), jnp.int32),
            vmem((heads * seqs, cols), F32),
            vmem((heads * seqs, nope), F32),
            vmem((n, QPARTS, seqs // pack * heads // QPARTS, lanes), BF16),
            vmem((seqs, heads, width // 2), BF16),
            vmem((seqs, heads, width // 2), BF16),
            vmem((seqs, heads, 128), BF16),
            vmem((slots * (page + 8), 128), F32),
            vmem((slots, page, 128), BF16),
            vmem((nch + 1, heads, width), F32),
            vmem((nch + 1, heads, 128), F32),
            vmem((nch + 1, heads, 128), F32),
            vmem((seqs, heads, 128), F32),
            vmem((nch, heads, GROUP * page), F32),
            vmem((n, rows, width), BF16),
            vmem((n, 2 * hs, 128), F32),
            vmem((line, rows, width), BF16),
            vmem((line, 2 * hs, 128), F32),
            vmem((line, rows, width), BF16),
            vmem((line, 2 * hs, 128), F32),
            vmem((line, rows, width), BF16),
            vmem((line, 2 * hs, 128), F32),
            vmem((width // 128, rows, 128), F32),
            vmem((n, hs, cols, vdim), BF16),
            vmem((n, seqs, hs * vdim), BF16),
            vmem((seqs, wide // 2), F32),
            vmem((seqs, wide // 2), F32),
            dma((8,)), dma((2 * bulk,)),
            dma((QPARTS * line,)), dma((QPARTS * line,)), dma((QPARTS * line,)), dma((QPARTS * line,)),
            dma((n,)), dma((n,)), dma((n,)), dma((n,)),
            dma((line,)), dma((line,)), dma((line,)), dma((line,)),
            dma((line,)), dma((line,)), dma((line,)), dma((line,)),
            dma((n,)), dma((n,)), dma, dma,
        ],
        compiler_params=pltpu.CompilerParams(
            has_side_effects=True, collective_id=1, vmem_limit_bytes=60 * 1024 * 1024),
        name="decode",
    )(lengths, page_table, rope_cache, q_nope, w_uk.transpose(0, 2, 1), q_rope, latent_cache, value_up_weight, w_out)


def solution(mesh):
    return jax.shard_map(
        functools.partial(local, mesh.shape["seq"], mesh.shape["groups"]),
        mesh=mesh,
        in_specs=(
            P(("groups", "seq"), None, None),
            P(("groups", "seq"), None),
            P("groups", "mp", None),
            P("groups", "mp", None),
            P("mp", None, "seq"),
            P("mp", "seq", None),
            P("mp", "seq"),
            P("groups", None),
            P("groups"),
        ),
        out_specs=P("groups", ("seq", "mp")),
        check_vma=False,
    )
```

```python
import functools
import math

import jax
import jax.numpy as jnp
from jax import lax
from jax.experimental import pallas as pl
from jax.experimental.pallas import tpu as pltpu
from jax.sharding import PartitionSpec as P

NEG = -1e30
MESH = pl.DeviceIdType.MESH
GROUP = 4
UNROLL = 20
UNROLL1 = 10
QPARTS = 2
F32 = jnp.float32
BF16 = jnp.bfloat16


def make_plan(first_slot, page, lengths_ref, table_ref, plan_ref):
    seqs, pages = table_ref.shape
    slots_dev, wide = first_slot[1], plan_ref.shape[1]
    table = table_ref[...].astype(F32).T
    logical = lax.broadcasted_iota(jnp.int32, (pages, 1), 0)
    slot = lax.broadcasted_iota(jnp.int32, (pages, slots_dev), 1) + first_slot[0]
    slot = slot.astype(F32)
    fill = []
    for b in range(seqs):
        inside = jnp.clip(lengths_ref[b] - page * logical, 0, page)
        hit = table[:, b:b + 1] == slot
        fill.append(jnp.sum(jnp.where(hit, inside, 0), axis=0, keepdims=True))
    eye = (lax.broadcasted_iota(jnp.int32, (slots_dev, slots_dev), 0)
           == lax.broadcasted_iota(jnp.int32, (slots_dev, slots_dev), 1))
    earlier = (lax.broadcasted_iota(jnp.int32, (slots_dev, slots_dev), 1)
               < lax.broadcasted_iota(jnp.int32, (slots_dev, slots_dev), 0))
    at = lax.broadcasted_iota(jnp.int32, (1, wide), 1)
    start = jnp.zeros((1, 1), jnp.int32)
    owner = jnp.zeros((1, wide), jnp.int32)
    fresh = jnp.zeros((1, wide), jnp.int32)
    entry = jnp.zeros((1, wide), jnp.int32)
    target = jnp.full((slots_dev, 1), -1, jnp.int32)
    column = jnp.zeros((slots_dev, 1), jnp.int32)
    for b in range(seqs):
        owned = fill[b] > 0
        count = jnp.sum(owned.astype(jnp.int32), axis=1, keepdims=True)
        place = jnp.sum(jnp.where(earlier & owned, 1, 0), axis=1, keepdims=True)
        mine = jnp.sum(jnp.where(eye, fill[b], 0), axis=1, keepdims=True)
        target = jnp.where(mine > 0, start * GROUP + place, target)
        column = column + mine
        fresh = jnp.where(at == start, 1, fresh)
        start = start + (count + GROUP - 1) // GROUP
        owner = owner + (at >= start).astype(jnp.int32)
        entry = jnp.where((at == b) & (count > 0), start, entry)
    match = target == lax.broadcasted_iota(jnp.int32, (slots_dev, wide), 1)
    ids = lax.broadcasted_iota(jnp.int32, (slots_dev, wide), 0)
    plan_ref[0:1, :] = jnp.sum(jnp.where(match, ids, 0), axis=0, keepdims=True)
    plan_ref[1:2, :] = jnp.sum(jnp.where(match, column, 0), axis=0, keepdims=True)
    plan_ref[2:3, :] = jnp.minimum(owner, seqs - 1)
    plan_ref[3:4, :] = fresh
    plan_ref[4:5, :] = entry
    plan_ref[5:8, :] = jnp.zeros((3, wide), jnp.int32)


def weigh(seqs, stats):
    hs = stats[0].shape[0] // 2
    tops = [s[:hs] for s in stats]
    best = functools.reduce(jnp.maximum, tops)
    shares = [s[hs:] * jnp.exp2(t - best) for s, t in zip(stats, tops)]
    total = functools.reduce(jnp.add, shares)
    inv = 1.0 / jnp.maximum(total, 1e-30)
    columns = []
    for share in shares:
        share = share * inv
        columns.append(jnp.concatenate([share[:, b:b + 1] for b in range(seqs)], axis=0))
    return columns, best, total


def mean(columns, parts):
    return functools.reduce(jnp.add, [p.astype(F32) * c for c, p in zip(columns, parts)])


def kernel(n, groups, pack, scale, nch,
           lengths_hbm, table_hbm, rope_hbm, qn_hbm, wuk_hbm, qr_hbm, lat_hbm, v_hbm, w_hbm, out_ref,
           lengths, table, rope, qn, wuk, qr, lat, w_buf, plan_v, plan, raw, flat, gath, q_near, q_far, turn,
           wide_rope, spread, run, tops, sums, peak, part, wts, mix, st, ygot, yst, zout, zst, zgot, zgst, port,
           vbuf, vals, tx, rx,
           lsem, bulk, qs1, qr1, qs2, qr2, vs1, vr1, vs2, vr2, ys, yr, yss, ysr, zs, zr, zss, zsr, as_, ar, ms, mr):
    me = lax.axis_index("seq")
    half = lax.axis_index("mp")
    grp = lax.axis_index("groups")
    seqs, heads, _ = qn.shape
    cols = wuk.shape[1]
    _, slots, page, wing = lat.shape
    width = 2 * wing
    hs = heads // n
    line = n // 2
    par = lax.rem(me, 2)
    row = me // 2
    partner = me + 1 - 2 * par
    share = groups == 2 and hs % 2 == 0
    hh = hs // 2 if share else hs
    voff = grp * hh if share else 0
    hp = heads // QPARTS
    near_n = line // 2
    side, pos = row // near_n, lax.rem(row, near_n)

    def along_of(j, sign):
        other, k = (0, j) if j < near_n else (1, j - near_n)
        at = lax.rem(pos + sign * k + near_n, near_n)
        return 2 * ((side + other * (1 - 2 * side)) * near_n + at) + par

    rows_out = []
    for j in range(line - 1):
        down = jnp.where(line - 1 - j > row, line - 1 - j, line - 2 - j)
        rows_out.append(jnp.where(side == 0, down, jnp.where(row > j, j, j + 1)))
    peers = [2 * r + par for r in rows_out] + [2 * r + 1 - par for r in rows_out] + [partner]

    barrier = pltpu.get_barrier_semaphore()
    for k in range(1, n):
        pl.semaphore_signal(barrier, inc=1, device_id={"seq": lax.rem(me + k, n)}, device_id_type=MESH)
    pl.semaphore_signal(barrier, inc=1, device_id={"mp": 1 - half}, device_id_type=MESH)
    if share:
        pl.semaphore_signal(barrier, inc=1, device_id={"groups": 1 - grp}, device_id_type=MESH)

    loads = [pltpu.make_async_copy(a, b, lsem.at[i]) for i, (a, b) in enumerate((
        (qn_hbm, qn), (wuk_hbm.at[pl.ds(0, hp)], wuk.at[pl.ds(0, hp)]), (lengths_hbm, lengths), (table_hbm, table), (qr_hbm, qr), (rope_hbm, rope)) + tuple(
            (wuk_hbm.at[pl.ds(i * hp, hp)], wuk.at[pl.ds(i * hp, hp)]) for i in range(1, QPARTS)))]
    for i in (0, 1, *range(6, len(loads)), 2, 3, 4, 5):
        loads[i].start()
    nb = bulk.shape[0] // 2
    step_l = 2 * slots // nb
    big = [pltpu.make_async_copy(
        lat_hbm.at[pl.ds(i // 2 * step_l, step_l), :, pl.ds(i % 2 * wing, wing)],
        lat.at[i % 2, pl.ds(i // 2 * step_l, step_l)], bulk.at[i]) for i in range(nb)]
    step_w = w_buf.shape[0] // nb
    bigw = [pltpu.make_async_copy(w_hbm.at[pl.ds(i * step_w, step_w)], w_buf.at[pl.ds(i * step_w, step_w)], bulk.at[nb + i])
            for i in range(nb)]
    own_v = pltpu.make_async_copy(v_hbm.at[pl.ds(me * hs, hs)], vbuf.at[me], lsem.at[5 + QPARTS])

    def remote(src, dst, s, r, where):
        return pltpu.make_async_remote_copy(
            src_ref=src, dst_ref=dst, send_sem=s, recv_sem=r, device_id=where, device_id_type=MESH)

    loads[0].wait()
    for b in range(seqs):
        flat[b * heads:(b + 1) * heads, :] = qn[b].astype(F32)

    def q_copy(block, i, k, peer, s, r):
        return remote(gath.at[block, i], gath.at[block, i], s.at[i * line + k], r.at[i * line + k], {"seq": peer})

    along, across = [], []
    for i in range(QPARTS):
        loads[5 + i if i else 1].wait()
        if i == QPARTS - 1:
            for copy in big:
                copy.start()
        for h in range(i * hp, (i + 1) * hp):
            q = flat[pl.ds(h, seqs, stride=heads), :].astype(BF16)
            raw[h * seqs:(h + 1) * seqs, :] = lax.dot_general(
                q, wuk[h], (((1,), (1,)), ((), ())), preferred_element_type=F32)
        for p in range(seqs // pack):
            parts = [raw[pl.ds(i * hp * seqs + p * pack + j, hp, stride=seqs), :] for j in range(pack)]
            whole = parts[0] if pack == 1 else jnp.concatenate(parts, axis=1)
            gath[me, i, p * hp:(p + 1) * hp, :] = whole.astype(BF16)
        if i == 0:
            pl.semaphore_wait(barrier, n - 1 + 1 + int(share))
        for k in range(1, line):
            copy = q_copy(me, i, k, along_of(k, 1), qs1, qr1)
            copy.start()
            along.append((i, k, copy))
        copy = q_copy(me, i, 0, partner, qs2, qr2)
        copy.start()
        across.append((0, copy))

    def v_copy(d, s):
        return remote(v_hbm.at[pl.ds(d * hs + voff, hh)], vbuf.at[s, pl.ds(voff, hh)], vs1.at[d], vr1.at[s], {"seq": d})

    def twin_copy(s):
        return remote(vbuf.at[s, pl.ds(voff, hh)], vbuf.at[s, pl.ds(voff, hh)], vs2.at[s], vr2.at[s], {"groups": 1 - grp})

    def relay(sources):
        for s in sources if share else []:
            v_copy(s, s).wait_recv()
            twin_copy(s).start()

    loads[2].wait()
    loads[3].wait()
    make_plan((me * slots, slots), page, lengths, table, plan_v)
    plan_copy = pltpu.make_async_copy(plan_v, plan, lsem.at[6 + QPARTS])
    plan_copy.start()
    loads[4].wait()
    loads[5].wait()
    own_v.start()
    per = page * 128 // rope.shape[1]
    pitch = wide_rope.shape[0] // slots
    lane = lax.broadcasted_iota(jnp.int32, (slots, 128), 1) // (128 // per)

    def widen(i):
        x = rope[:, i * 128:(i + 1) * 128].astype(F32)
        for j in range(per):
            wide_rope[pl.ds(i * per + j, slots, stride=pitch), :] = jnp.where(lane == j, x, 0.0)

    def narrow(i, _):
        spread[i] = wide_rope[pl.ds(pl.multiple_of(i * pitch, 8), page), :].astype(BF16)
        return 0

    along.sort(key=lambda x: (x[1] >= near_n, x[0], x[1]))
    steps = rope.shape[1] // 128
    share_w = -(-steps // max(1, len(along) // 2))
    for i, (q, k, copy) in enumerate(along):
        for f in range(min(steps, i * share_w), min(steps, (i + 1) * share_w)):
            widen(f)
        if (i + 1) * share_w >= steps > i * share_w:
            lax.fori_loop(0, slots, narrow, 0, unroll=4)
        copy.wait_recv()
        forward = q_copy(along_of(k, -1), q, k, partner, qs2, qr2)
        forward.start()
        across.append((k, forward))

    for d in peers:
        v_copy(d, me).start()

    for b in range(seqs):
        turn[b] = jnp.concatenate([qr[b]] * (128 // qr.shape[2]), axis=1)
    for j in range(2):
        run[j, 0] = jnp.zeros(run.shape[2:], F32)
    tops[0] = jnp.full(tops.shape[1:], NEG, F32)
    sums[0] = jnp.zeros(sums.shape[1:], F32)
    plan_copy.wait()
    for copy in big:
        copy.wait()
    for copy in bigw:
        copy.start()

    def assemble(first, dst):
        for i in range(QPARTS):
            for s in range(n // 2):
                for b in range(seqs):
                    at = b % pack * cols
                    dst[b, i * hp:(i + 1) * hp, s * cols:(s + 1) * cols] = gath[
                        first + s, i, b // pack * hp:(b // pack + 1) * hp, at:at + cols]

    tokens = GROUP * page
    tlane = lax.broadcasted_iota(jnp.int32, (1, tokens), 1)
    nt = (((1,), (1,)), ((), ()))

    def slots_of(ref, c):
        return jnp.concatenate([ref[plan[0, c * GROUP + g]] for g in range(GROUP)], axis=0)

    def first_pass(it, _):
        for u in range(UNROLL1):
            c = it * UNROLL1 + u
            b = plan[2, c]
            limit = jnp.zeros((1, tokens), jnp.int32)
            for g in range(GROUP):
                limit = jnp.where(tlane // page == g, plan[1, c * GROUP + g] + g * page, limit)
            score = lax.dot_general(turn[b], slots_of(spread, c), nt, preferred_element_type=F32)
            score = score + lax.dot_general(q_near[b], slots_of(lat.at[side], c), nt, preferred_element_type=F32)
            part[c] = jnp.where(tlane < limit, score, NEG)
        return 0

    for k, copy in across:
        if k < near_n:
            copy.wait_recv()
    assemble(side * (n // 2), q_near)
    trips = nch // UNROLL
    lax.fori_loop(0, nch // UNROLL1, first_pass, 0)
    for k, copy in across:
        if k >= near_n:
            copy.wait_recv()
    assemble((1 - side) * (n // 2), q_far)

    def second_pass(it, _):
        top = tops[it * UNROLL]
        for u in range(UNROLL):
            c = it * UNROLL + u
            far = lax.dot_general(q_far[plan[2, c]], slots_of(lat.at[1 - side], c), nt, preferred_element_type=F32)
            score = (part[c] + far) * scale
            part[c] = score
            top = jnp.where(plan[3, c] > 0, NEG, top)
            for j in range(tokens // 128):
                top = jnp.maximum(top, score[:, j * 128:(j + 1) * 128])
            tops[c + 1] = top
        return 0

    lax.fori_loop(0, trips, second_pass, 0)
    for b in range(seqs):
        peak[b] = jnp.broadcast_to(jnp.max(tops[plan[4, b]], axis=1, keepdims=True), peak.shape[1:])

    def third_pass(it, _):
        acc, total = run[0, it * UNROLL], sums[it * UNROLL]
        for u in range(UNROLL):
            c = it * UNROLL + u
            top = peak[plan[2, c]]
            keep = jnp.where(plan[3, c] > 0, 0.0, 1.0)
            weight = [jnp.exp2(part[c, :, j * 128:(j + 1) * 128] - top) for j in range(tokens // 128)]
            total = total * keep + functools.reduce(jnp.add, weight)
            weight = jnp.concatenate([x.astype(BF16) for x in weight], axis=1)
            wts[c] = weight
            acc = acc * keep + jnp.dot(weight, slots_of(lat.at[0], c), preferred_element_type=F32)
            sums[c + 1] = total
            run[0, c + 1] = acc
        return 0

    def fourth_pass(it, _):
        acc = run[1, it * UNROLL]
        for u in range(UNROLL):
            c = it * UNROLL + u
            keep = jnp.where(plan[3, c] > 0, 0.0, 1.0)
            acc = acc * keep + jnp.dot(wts[c], slots_of(lat.at[1], c), preferred_element_type=F32)
            run[1, c + 1] = acc
        return 0

    ids = lax.broadcasted_iota(jnp.int32, (heads, 128), 1)
    everyone = rows_out + [row]

    def pack_sums(j):
        all_top = jnp.full((heads, 128), NEG, F32)
        all_sum = jnp.zeros((heads, 128), F32)
        for p in range(seqs // 2):
            pair = []
            for b in (2 * p, 2 * p + 1):
                entry = plan[4, b]
                total = jnp.sum(sums[entry], axis=1, keepdims=True)
                all_top = jnp.where(ids == b, peak[b], all_top)
                all_sum = jnp.where(ids == b, total, all_sum)
                pair.append(run[j, entry] * (1.0 / jnp.maximum(total, 1e-30)))
            for d in range(n):
                mix[j, d, 2 * p * hs:2 * (p + 1) * hs, :] = jnp.concatenate(
                    [x[d * hs:(d + 1) * hs] for x in pair], axis=0).astype(BF16)
        if j == 0:
            for d in range(n):
                st[d, :hs, :] = all_top[d * hs:(d + 1) * hs]
                st[d, hs:, :] = all_sum[d * hs:(d + 1) * hs]

    ysent = {}

    def to_partner(j, places):
        for i in places:
            r = everyone[i]
            d = 2 * r + 1 - par
            if j == 0:
                ysent[2, i] = remote(st.at[d], yst.at[r], yss.at[i], ysr.at[i], {"seq": partner})
                ysent[2, i].start()
            ysent[j, i] = remote(mix.at[j, d], ygot.at[j, r], ys.at[j * line + i], yr.at[j * line + i], {"seq": partner})
            ysent[j, i].start()

    lax.fori_loop(0, trips, third_pass, 0)
    pack_sums(0)
    to_partner(0, range(line - 1))
    relay(peers[:line - 1][::-1])
    lax.fori_loop(0, trips, fourth_pass, 0)
    pack_sums(1)
    to_partner(1, range(line - 1))
    to_partner(0, [line - 1])
    to_partner(1, [line - 1])
    onward = []
    for j, i in [(j, i) for j in range(2) for i in range(line - 1)] + [(0, line - 1), (1, line - 1)]:
        r = everyone[i]
        if j == 0:
            ysent[2, i].wait_recv()
        ysent[j, i].wait_recv()
        mine = 2 * r + par
        columns, best, total = weigh(seqs, [st[mine], yst[r]])
        zout[j, i] = mean(columns, [mix[j, mine], ygot[j, r]]).astype(BF16)
        moves = [(zout.at[j, i], zgot.at[j, row], zs.at[j * line + i], zr.at[j * line + row])]
        if j == 0:
            zst[i, :hs, :] = best
            zst[i, hs:, :] = total
            moves.append((zst.at[i], zgst.at[row], zss.at[i], zsr.at[row]))
        if i < line - 1:
            for move in moves:
                copy = remote(*move, {"seq": 2 * r + par})
                copy.start()
                onward.append(copy)
        relay(peers[line - 1:][i + j * (line - 1):i + j * (line - 1) + 1] if i < line - 1 else [])
    blocks = wing // 128
    for j in range(2):
        for r in rows_out:
            if j == 0:
                remote(zst.at[0], zgst.at[r], zss.at[0], zsr.at[r], {"seq": partner}).wait_recv()
            remote(zout.at[j, 0], zgot.at[j, r], zs.at[0], zr.at[j * line + r], {"seq": partner}).wait_recv()
        columns, _, _ = weigh(seqs, [zst[line - 1]] + [zgst[r] for r in rows_out])
        o = mean(columns, [zout[j, line - 1]] + [zgot[j, r] for r in rows_out])
        for i in range(blocks):
            port[j * blocks + i] = o[:, i * 128:(i + 1) * 128]

    own_v.wait()
    for d in peers:
        if share:
            twin_copy(d).wait_recv()
        else:
            v_copy(d, d).wait_recv()
    vdim = vbuf.shape[3]
    for h in range(hs):
        x = jnp.concatenate([port[j, pl.ds(h, seqs, stride=hs), :] for j in range(2 * blocks)], axis=1).astype(BF16)
        wv = vbuf[:, h].reshape(width, vdim)
        vals[me, :, h * vdim:(h + 1) * vdim] = jnp.dot(x, wv, preferred_element_type=F32).astype(BF16)
    copies = []
    for i in [x for j in range(line - 1) for x in (line - 1 + j, j)] + [n - 2]:
        copy = remote(vals.at[me], vals.at[me], as_.at[i], ar.at[me], {"seq": peers[i]})
        copy.start()
        copies.append(copy)
    for copy in bigw:
        copy.wait()
    rows = hs * vdim
    res = None
    for src in [me, partner] + [peers[i] for j in range(line - 2, -1, -1) for i in (j, line - 1 + j)]:
        if src is not me:
            remote(vals.at[src], vals.at[src], as_.at[0], ar.at[src], {"seq": partner}).wait_recv()
        at = pl.ds(pl.multiple_of(src * rows, rows), rows)
        product = jnp.dot(vals[src], w_buf[at, :], preferred_element_type=F32)
        res = product if res is None else res + product
    wide = res.shape[1] // 2
    low, high = res[:, :wide], res[:, wide:]
    first = half == 0
    tx[...] = jnp.where(first, high, low)
    copy = remote(tx, rx, ms, mr, {"mp": 1 - half})
    copy.start()
    for c in copies + list(ysent.values()) + onward + [x[2] for x in along] + [x[1] for x in across]:
        c.wait_send()
    for d in peers:
        v_copy(d, me).wait_send()
        if share:
            twin_copy(d).wait_send()
    copy.wait()
    out_ref[...] = (jnp.where(first, low, high) + rx[...]).astype(BF16)


def local(n, groups, latent_cache, rope_cache, q_nope, q_rope, w_uk, value_up_weight, w_out, page_table, lengths):
    slots, page, width = latent_cache.shape
    seqs, heads, nope = q_nope.shape
    rope_w = q_rope.shape[2]
    cols = w_uk.shape[2]
    vdim = value_up_weight.shape[2]
    scale = (nope + rope_w) ** (-0.5) * math.log2(math.e)
    pack = max(1, min(seqs, 128 // cols))
    lanes = pack * cols
    hs = heads // n
    line = n // 2
    rows = seqs * hs
    wide = w_out.shape[1]
    nch = (slots + seqs * (GROUP - 1)) // GROUP
    nch = -(-nch // UNROLL) * UNROLL
    pw = (nch * GROUP + 127) // 128 * 128
    vm = pl.BlockSpec(memory_space=pltpu.VMEM)
    hbm = pl.BlockSpec(memory_space=pl.ANY)
    dma = pltpu.SemaphoreType.DMA
    vmem = pltpu.VMEM
    bulk = 8
    return pl.pallas_call(
        functools.partial(kernel, n, groups, pack, scale, nch),
        out_shape=jax.ShapeDtypeStruct((seqs, wide // 2), BF16),
        in_specs=[hbm] * 9, out_specs=vm,
        scratch_shapes=[
            pltpu.SMEM(lengths.shape, jnp.int32),
            vmem(page_table.shape, jnp.int32),
            vmem(rope_cache.shape, BF16),
            vmem(q_nope.shape, BF16),
            vmem((heads, cols, nope), BF16),
            vmem(q_rope.shape, BF16),
            vmem((2, slots, page, width // 2), BF16),
            vmem(w_out.shape, BF16),
            vmem((8, pw), jnp.int32),
            pltpu.SMEM((8, pw), jnp.int32),
            vmem((heads * seqs, cols), F32),
            vmem((heads * seqs, nope), F32),
            vmem((n, QPARTS, seqs // pack * heads // QPARTS, lanes), BF16),
            vmem((seqs, heads, width // 2), BF16),
            vmem((seqs, heads, width // 2), BF16),
            vmem((seqs, heads, 128), BF16),
            vmem((slots * (page + 8), 128), F32),
            vmem((slots, page, 128), BF16),
            vmem((2, nch + 1, heads, width // 2), F32),
            vmem((nch + 1, heads, 128), F32),
            vmem((nch + 1, heads, 128), F32),
            vmem((seqs, heads, 128), F32),
            vmem((nch, heads, GROUP * page), F32),
            vmem((nch, heads, GROUP * page), BF16),
            vmem((2, n, rows, width // 2), BF16),
            vmem((n, 2 * hs, 128), F32),
            vmem((2, line, rows, width // 2), BF16),
            vmem((line, 2 * hs, 128), F32),
            vmem((2, line, rows, width // 2), BF16),
            vmem((line, 2 * hs, 128), F32),
            vmem((2, line, rows, width // 2), BF16),
            vmem((line, 2 * hs, 128), F32),
            vmem((width // 128, rows, 128), F32),
            vmem((n, hs, cols, vdim), BF16),
            vmem((n, seqs, hs * vdim), BF16),
            vmem((seqs, wide // 2), F32),
            vmem((seqs, wide // 2), F32),
            dma((7 + QPARTS,)), dma((2 * bulk,)),
            dma((QPARTS * line,)), dma((QPARTS * line,)), dma((QPARTS * line,)), dma((QPARTS * line,)),
            dma((n,)), dma((n,)), dma((n,)), dma((n,)),
            dma((2 * line,)), dma((2 * line,)), dma((line,)), dma((line,)),
            dma((2 * line,)), dma((2 * line,)), dma((line,)), dma((line,)),
            dma((n,)), dma((n,)), dma, dma,
        ],
        compiler_params=pltpu.CompilerParams(
            has_side_effects=True, collective_id=1, vmem_limit_bytes=60 * 1024 * 1024),
        name="decode",
    )(lengths, page_table, rope_cache, q_nope, w_uk.transpose(0, 2, 1), q_rope, latent_cache, value_up_weight, w_out)


def solution(mesh):
    return jax.shard_map(
        functools.partial(local, mesh.shape["seq"], mesh.shape["groups"]),
        mesh=mesh,
        in_specs=(
            P(("groups", "seq"), None, None),
            P(("groups", "seq"), None),
            P("groups", "mp", None),
            P("groups", "mp", None),
            P("mp", None, "seq"),
            P("mp", "seq", None),
            P("mp", "seq"),
            P("groups", None),
            P("groups"),
        ),
        out_specs=P("groups", ("seq", "mp")),
        check_vma=False,
    )
```

```python
import functools
import math

import jax
import jax.numpy as jnp
from jax import lax
from jax.experimental import pallas as pl
from jax.experimental.pallas import tpu as pltpu
from jax.sharding import PartitionSpec as P

NEG = -1e30
MESH = pl.DeviceIdType.MESH
GROUP = 4
UNROLL = 19
UNROLL1 = 19
QPARTS = 2
F32 = jnp.float32
BF16 = jnp.bfloat16


def make_plan(first_slot, page, lengths_ref, table_ref, plan_ref):
    seqs, pages = table_ref.shape
    slots_dev, wide = first_slot[1], plan_ref.shape[1]
    table = table_ref[...].astype(F32).T
    logical = lax.broadcasted_iota(jnp.int32, (pages, 1), 0)
    slot = lax.broadcasted_iota(jnp.int32, (pages, slots_dev), 1) + first_slot[0]
    slot = slot.astype(F32)
    fill = []
    for b in range(seqs):
        inside = jnp.clip(lengths_ref[b] - page * logical, 0, page)
        hit = table[:, b:b + 1] == slot
        fill.append(jnp.sum(jnp.where(hit, inside, 0), axis=0, keepdims=True))
    eye = (lax.broadcasted_iota(jnp.int32, (slots_dev, slots_dev), 0)
           == lax.broadcasted_iota(jnp.int32, (slots_dev, slots_dev), 1))
    earlier = (lax.broadcasted_iota(jnp.int32, (slots_dev, slots_dev), 1)
               < lax.broadcasted_iota(jnp.int32, (slots_dev, slots_dev), 0))
    at = lax.broadcasted_iota(jnp.int32, (1, wide), 1)
    start = jnp.zeros((1, 1), jnp.int32)
    owner = jnp.zeros((1, wide), jnp.int32)
    fresh = jnp.zeros((1, wide), jnp.int32)
    entry = jnp.zeros((1, wide), jnp.int32)
    target = jnp.full((slots_dev, 1), -1, jnp.int32)
    column = jnp.zeros((slots_dev, 1), jnp.int32)
    for b in range(seqs):
        owned = fill[b] > 0
        count = jnp.sum(owned.astype(jnp.int32), axis=1, keepdims=True)
        place = jnp.sum(jnp.where(earlier & owned, 1, 0), axis=1, keepdims=True)
        mine = jnp.sum(jnp.where(eye, fill[b], 0), axis=1, keepdims=True)
        target = jnp.where(mine > 0, start * GROUP + place, target)
        column = column + mine
        fresh = jnp.where(at == start, 1, fresh)
        start = start + (count + GROUP - 1) // GROUP
        owner = owner + (at >= start).astype(jnp.int32)
        entry = jnp.where((at == b) & (count > 0), start, entry)
    match = target == lax.broadcasted_iota(jnp.int32, (slots_dev, wide), 1)
    ids = lax.broadcasted_iota(jnp.int32, (slots_dev, wide), 0)
    plan_ref[0:1, :] = jnp.sum(jnp.where(match, ids, 0), axis=0, keepdims=True)
    plan_ref[1:2, :] = jnp.sum(jnp.where(match, column, 0), axis=0, keepdims=True)
    plan_ref[2:3, :] = jnp.minimum(owner, seqs - 1)
    plan_ref[3:4, :] = fresh
    plan_ref[4:5, :] = entry
    plan_ref[5:8, :] = jnp.zeros((3, wide), jnp.int32)


def weigh(seqs, stats):
    hs = stats[0].shape[0] // 2
    tops = [s[:hs] for s in stats]
    best = functools.reduce(jnp.maximum, tops)
    shares = [s[hs:] * jnp.exp2(t - best) for s, t in zip(stats, tops)]
    total = functools.reduce(jnp.add, shares)
    inv = 1.0 / jnp.maximum(total, 1e-30)
    columns = []
    for share in shares:
        share = share * inv
        columns.append(jnp.concatenate([share[:, b:b + 1] for b in range(seqs)], axis=0))
    return columns, best, total


def mean(columns, parts):
    return functools.reduce(jnp.add, [p.astype(F32) * c for c, p in zip(columns, parts)])


def kernel(n, groups, pack, scale, nch,
           lengths_hbm, table_hbm, rope_hbm, qn_hbm, wuk_hbm, qr_hbm, lat_hbm, v_hbm, w_hbm, out_ref,
           lengths, table, rope, qn, wuk, qr, lat, w_buf, plan_v, plan, raw, flat, gath, q_near, q_far, turn,
           wide_rope, spread, run, tops, sums, peak, part, wts, mix, st, ygot, yst, zout, zst, zgot, zgst, port,
           vbuf, vals, tx, rx,
           lsem, bulk, qs1, qr1, qs2, qr2, vs1, vr1, vs2, vr2, ys, yr, yss, ysr, zs, zr, zss, zsr, as_, ar, ms, mr):
    me = lax.axis_index("seq")
    half = lax.axis_index("mp")
    grp = lax.axis_index("groups")
    seqs, heads, _ = qn.shape
    cols = wuk.shape[1]
    _, slots, page, wing = lat.shape
    width = 2 * wing
    hs = heads // n
    line = n // 2
    par = lax.rem(me, 2)
    row = me // 2
    partner = me + 1 - 2 * par
    share = groups == 2 and hs % 2 == 0
    hh = hs // 2 if share else hs
    voff = grp * hh if share else 0
    hp = heads // QPARTS
    near_n = line // 2
    side, pos = row // near_n, lax.rem(row, near_n)

    def along_of(j, sign):
        other, k = (0, j) if j < near_n else (1, j - near_n)
        at = lax.rem(pos + sign * k + near_n, near_n)
        return 2 * ((side + other * (1 - 2 * side)) * near_n + at) + par

    rows_out = []
    for j in range(line - 1):
        down = jnp.where(line - 1 - j > row, line - 1 - j, line - 2 - j)
        rows_out.append(jnp.where(side == 0, down, jnp.where(row > j, j, j + 1)))
    peers = [2 * r + par for r in rows_out] + [2 * r + 1 - par for r in rows_out] + [partner]

    barrier = pltpu.get_barrier_semaphore()
    for k in range(1, n):
        pl.semaphore_signal(barrier, inc=1, device_id={"seq": lax.rem(me + k, n)}, device_id_type=MESH)
    pl.semaphore_signal(barrier, inc=1, device_id={"mp": 1 - half}, device_id_type=MESH)
    if share:
        pl.semaphore_signal(barrier, inc=1, device_id={"groups": 1 - grp}, device_id_type=MESH)

    loads = [pltpu.make_async_copy(a, b, lsem.at[i]) for i, (a, b) in enumerate((
        (qn_hbm, qn), (wuk_hbm.at[pl.ds(0, hp)], wuk.at[pl.ds(0, hp)]), (lengths_hbm, lengths), (table_hbm, table), (qr_hbm, qr), (rope_hbm, rope)) + tuple(
            (wuk_hbm.at[pl.ds(i * hp, hp)], wuk.at[pl.ds(i * hp, hp)]) for i in range(1, QPARTS)))]
    for i in (0, 1, *range(6, len(loads)), 2, 3, 4, 5):
        loads[i].start()
    nb = bulk.shape[0] // 2
    step_l = 2 * slots // nb
    big = [pltpu.make_async_copy(
        lat_hbm.at[pl.ds(i // 2 * step_l, step_l), :, pl.ds(i % 2 * wing, wing)],
        lat.at[i % 2, pl.ds(i // 2 * step_l, step_l)], bulk.at[i]) for i in range(nb)]
    step_w = w_buf.shape[0] // nb
    bigw = [pltpu.make_async_copy(w_hbm.at[pl.ds(i * step_w, step_w)], w_buf.at[pl.ds(i * step_w, step_w)], bulk.at[nb + i])
            for i in range(nb)]
    own_v = pltpu.make_async_copy(v_hbm.at[pl.ds(me * hs, hs)], vbuf.at[me], lsem.at[5 + QPARTS])

    def remote(src, dst, s, r, where):
        return pltpu.make_async_remote_copy(
            src_ref=src, dst_ref=dst, send_sem=s, recv_sem=r, device_id=where, device_id_type=MESH)

    loads[0].wait()
    for b in range(seqs):
        flat[b * heads:(b + 1) * heads, :] = qn[b].astype(F32)

    def q_copy(block, i, k, peer, s, r):
        return remote(gath.at[block, i], gath.at[block, i], s.at[i * line + k], r.at[i * line + k], {"seq": peer})

    along, across = [], []
    for i in range(QPARTS):
        loads[5 + i if i else 1].wait()
        if i == QPARTS - 1:
            for copy in big:
                copy.start()
        for h in range(i * hp, (i + 1) * hp):
            q = flat[pl.ds(h, seqs, stride=heads), :].astype(BF16)
            raw[h * seqs:(h + 1) * seqs, :] = lax.dot_general(
                q, wuk[h], (((1,), (1,)), ((), ())), preferred_element_type=F32)
        for p in range(seqs // pack):
            parts = [raw[pl.ds(i * hp * seqs + p * pack + j, hp, stride=seqs), :] for j in range(pack)]
            whole = parts[0] if pack == 1 else jnp.concatenate(parts, axis=1)
            gath[me, i, p * hp:(p + 1) * hp, :] = whole.astype(BF16)
        if i == 0:
            pl.semaphore_wait(barrier, n - 1 + 1 + int(share))
        for k in range(1, line):
            copy = q_copy(me, i, k, along_of(k, 1), qs1, qr1)
            copy.start()
            along.append((i, k, copy))
        copy = q_copy(me, i, 0, partner, qs2, qr2)
        copy.start()
        across.append((0, copy))

    def v_copy(d, s):
        return remote(v_hbm.at[pl.ds(d * hs + voff, hh)], vbuf.at[s, pl.ds(voff, hh)], vs1.at[d], vr1.at[s], {"seq": d})

    def twin_copy(s):
        return remote(vbuf.at[s, pl.ds(voff, hh)], vbuf.at[s, pl.ds(voff, hh)], vs2.at[s], vr2.at[s], {"groups": 1 - grp})

    def relay(sources):
        for s in sources if share else []:
            v_copy(s, s).wait_recv()
            twin_copy(s).start()

    loads[2].wait()
    loads[3].wait()
    make_plan((me * slots, slots), page, lengths, table, plan_v)
    plan_copy = pltpu.make_async_copy(plan_v, plan, lsem.at[6 + QPARTS])
    plan_copy.start()
    loads[4].wait()
    loads[5].wait()
    own_v.start()
    per = page * 128 // rope.shape[1]
    pitch = wide_rope.shape[0] // slots
    lane = lax.broadcasted_iota(jnp.int32, (slots, 128), 1) // (128 // per)

    def widen(i):
        x = rope[:, i * 128:(i + 1) * 128].astype(F32)
        for j in range(per):
            wide_rope[pl.ds(i * per + j, slots, stride=pitch), :] = jnp.where(lane == j, x, 0.0)

    def narrow(i, _):
        spread[i] = wide_rope[pl.ds(pl.multiple_of(i * pitch, 8), page), :].astype(BF16)
        return 0

    along.sort(key=lambda x: (x[1] >= near_n, x[0], x[1]))
    steps = rope.shape[1] // 128
    share_w = -(-steps // max(1, len(along) // 2))
    for i, (q, k, copy) in enumerate(along):
        for f in range(min(steps, i * share_w), min(steps, (i + 1) * share_w)):
            widen(f)
        if (i + 1) * share_w >= steps > i * share_w:
            lax.fori_loop(0, slots, narrow, 0, unroll=4)
        copy.wait_recv()
        forward = q_copy(along_of(k, -1), q, k, partner, qs2, qr2)
        forward.start()
        across.append((k, forward))

    for d in peers:
        v_copy(d, me).start()

    for b in range(seqs):
        turn[b] = jnp.concatenate([qr[b]] * (128 // qr.shape[2]), axis=1)
    for j in range(2):
        run[j, 0] = jnp.zeros(run.shape[2:], F32)
    tops[0] = jnp.full(tops.shape[1:], NEG, F32)
    sums[0] = jnp.zeros(sums.shape[1:], F32)
    plan_copy.wait()
    for copy in big:
        copy.wait()
    for copy in bigw:
        copy.start()

    def assemble(first, dst):
        for i in range(QPARTS):
            for s in range(n // 2):
                for b in range(seqs):
                    at = b % pack * cols
                    dst[b, i * hp:(i + 1) * hp, s * cols:(s + 1) * cols] = gath[
                        first + s, i, b // pack * hp:(b // pack + 1) * hp, at:at + cols]

    tokens = GROUP * page
    tlane = lax.broadcasted_iota(jnp.int32, (1, tokens), 1)
    nt = (((1,), (1,)), ((), ()))

    def slots_of(ref, c):
        return jnp.concatenate([ref[plan[0, c * GROUP + g]] for g in range(GROUP)], axis=0)

    def first_pass(it, _):
        for u in range(UNROLL1):
            c = it * UNROLL1 + u
            b = plan[2, c]
            limit = jnp.zeros((1, tokens), jnp.int32)
            for g in range(GROUP):
                limit = jnp.where(tlane // page == g, plan[1, c * GROUP + g] + g * page, limit)
            score = lax.dot_general(turn[b], slots_of(spread, c), nt, preferred_element_type=F32)
            score = score + lax.dot_general(q_near[b], slots_of(lat.at[side], c), nt, preferred_element_type=F32)
            part[c] = jnp.where(tlane < limit, score, NEG)
        return 0

    for k, copy in across:
        if k < near_n:
            copy.wait_recv()
    assemble(side * (n // 2), q_near)
    trips = nch // UNROLL
    lax.fori_loop(0, nch // UNROLL1, first_pass, 0)
    for k, copy in across:
        if k >= near_n:
            copy.wait_recv()
    assemble((1 - side) * (n // 2), q_far)

    def second_pass(it, _):
        top = tops[it * UNROLL]
        for u in range(UNROLL):
            c = it * UNROLL + u
            far = lax.dot_general(q_far[plan[2, c]], slots_of(lat.at[1 - side], c), nt, preferred_element_type=F32)
            score = (part[c] + far) * scale
            part[c] = score
            top = jnp.where(plan[3, c] > 0, NEG, top)
            for j in range(tokens // 128):
                top = jnp.maximum(top, score[:, j * 128:(j + 1) * 128])
            tops[c + 1] = top
        return 0

    lax.fori_loop(0, trips, second_pass, 0)
    for b in range(seqs):
        peak[b] = jnp.broadcast_to(jnp.max(tops[plan[4, b]], axis=1, keepdims=True), peak.shape[1:])

    def third_pass(it, _):
        acc, total = run[0, it * UNROLL], sums[it * UNROLL]
        for u in range(UNROLL):
            c = it * UNROLL + u
            top = peak[plan[2, c]]
            keep = jnp.where(plan[3, c] > 0, 0.0, 1.0)
            weight = [jnp.exp2(part[c, :, j * 128:(j + 1) * 128] - top) for j in range(tokens // 128)]
            total = total * keep + functools.reduce(jnp.add, weight)
            weight = jnp.concatenate([x.astype(BF16) for x in weight], axis=1)
            wts[c] = weight
            acc = acc * keep + jnp.dot(weight, slots_of(lat.at[0], c), preferred_element_type=F32)
            sums[c + 1] = total
            run[0, c + 1] = acc
        return 0

    def fourth_pass(it, _):
        acc = run[1, it * UNROLL]
        for u in range(UNROLL):
            c = it * UNROLL + u
            keep = jnp.where(plan[3, c] > 0, 0.0, 1.0)
            acc = acc * keep + jnp.dot(wts[c], slots_of(lat.at[1], c), preferred_element_type=F32)
            run[1, c + 1] = acc
        return 0

    ids = lax.broadcasted_iota(jnp.int32, (heads, 128), 1)
    everyone = rows_out + [row]

    def pack_sums(j):
        all_top = jnp.full((heads, 128), NEG, F32)
        all_sum = jnp.zeros((heads, 128), F32)
        for p in range(seqs // 2):
            pair = []
            for b in (2 * p, 2 * p + 1):
                entry = plan[4, b]
                total = jnp.sum(sums[entry], axis=1, keepdims=True)
                all_top = jnp.where(ids == b, peak[b], all_top)
                all_sum = jnp.where(ids == b, total, all_sum)
                pair.append(run[j, entry] * (1.0 / jnp.maximum(total, 1e-30)))
            for d in range(n):
                mix[j, d, 2 * p * hs:2 * (p + 1) * hs, :] = jnp.concatenate(
                    [x[d * hs:(d + 1) * hs] for x in pair], axis=0).astype(BF16)
        if j == 0:
            for d in range(n):
                st[d, :hs, :] = all_top[d * hs:(d + 1) * hs]
                st[d, hs:, :] = all_sum[d * hs:(d + 1) * hs]

    ysent = {}

    def to_partner(j, places):
        for i in places:
            r = everyone[i]
            d = 2 * r + 1 - par
            if j == 0:
                ysent[2, i] = remote(st.at[d], yst.at[r], yss.at[i], ysr.at[i], {"seq": partner})
                ysent[2, i].start()
            ysent[j, i] = remote(mix.at[j, d], ygot.at[j, r], ys.at[j * line + i], yr.at[j * line + i], {"seq": partner})
            ysent[j, i].start()

    lax.fori_loop(0, trips, third_pass, 0)
    pack_sums(0)
    to_partner(0, range(line - 1))
    relay(peers[:line - 1][::-1])
    lax.fori_loop(0, trips, fourth_pass, 0)
    pack_sums(1)
    to_partner(1, range(line - 1))
    to_partner(0, [line - 1])
    to_partner(1, [line - 1])
    onward = []
    for j, i in [(j, i) for j in range(2) for i in range(line - 1)] + [(0, line - 1), (1, line - 1)]:
        r = everyone[i]
        if j == 0:
            ysent[2, i].wait_recv()
        ysent[j, i].wait_recv()
        mine = 2 * r + par
        columns, best, total = weigh(seqs, [st[mine], yst[r]])
        zout[j, i] = mean(columns, [mix[j, mine], ygot[j, r]]).astype(BF16)
        moves = [(zout.at[j, i], zgot.at[j, row], zs.at[j * line + i], zr.at[j * line + row])]
        if j == 0:
            zst[i, :hs, :] = best
            zst[i, hs:, :] = total
            moves.append((zst.at[i], zgst.at[row], zss.at[i], zsr.at[row]))
        if i < line - 1:
            for move in moves:
                copy = remote(*move, {"seq": 2 * r + par})
                copy.start()
                onward.append(copy)
        relay(peers[line - 1:][i + j * (line - 1):i + j * (line - 1) + 1] if i < line - 1 else [])
    blocks = wing // 128
    for j in range(2):
        for r in rows_out:
            if j == 0:
                remote(zst.at[0], zgst.at[r], zss.at[0], zsr.at[r], {"seq": partner}).wait_recv()
            remote(zout.at[j, 0], zgot.at[j, r], zs.at[0], zr.at[j * line + r], {"seq": partner}).wait_recv()
        columns, _, _ = weigh(seqs, [zst[line - 1]] + [zgst[r] for r in rows_out])
        o = mean(columns, [zout[j, line - 1]] + [zgot[j, r] for r in rows_out])
        for i in range(blocks):
            port[j * blocks + i] = o[:, i * 128:(i + 1) * 128]

    own_v.wait()
    for d in peers:
        if share:
            twin_copy(d).wait_recv()
        else:
            v_copy(d, d).wait_recv()
    vdim = vbuf.shape[3]
    for h in range(hs):
        x = jnp.concatenate([port[j, pl.ds(h, seqs, stride=hs), :] for j in range(2 * blocks)], axis=1).astype(BF16)
        wv = vbuf[:, h].reshape(width, vdim)
        vals[me, :, h * vdim:(h + 1) * vdim] = jnp.dot(x, wv, preferred_element_type=F32).astype(BF16)
    copies = []
    for i in [x for j in range(line - 1) for x in (line - 1 + j, j)] + [n - 2]:
        copy = remote(vals.at[me], vals.at[me], as_.at[i], ar.at[me], {"seq": peers[i]})
        copy.start()
        copies.append(copy)
    for copy in bigw:
        copy.wait()
    rows = hs * vdim
    res = None
    for src in [me, partner] + [peers[i] for j in range(line - 2, -1, -1) for i in (j, line - 1 + j)]:
        if src is not me:
            remote(vals.at[src], vals.at[src], as_.at[0], ar.at[src], {"seq": partner}).wait_recv()
        at = pl.ds(pl.multiple_of(src * rows, rows), rows)
        product = jnp.dot(vals[src], w_buf[at, :], preferred_element_type=F32)
        res = product if res is None else res + product
    wide = res.shape[1] // 2
    low, high = res[:, :wide], res[:, wide:]
    first = half == 0
    tx[...] = jnp.where(first, high, low)
    copy = remote(tx, rx, ms, mr, {"mp": 1 - half})
    copy.start()
    for c in copies + list(ysent.values()) + onward + [x[2] for x in along] + [x[1] for x in across]:
        c.wait_send()
    for d in peers:
        v_copy(d, me).wait_send()
        if share:
            twin_copy(d).wait_send()
    copy.wait()
    out_ref[...] = (jnp.where(first, low, high) + rx[...]).astype(BF16)


def local(n, groups, latent_cache, rope_cache, q_nope, q_rope, w_uk, value_up_weight, w_out, page_table, lengths):
    slots, page, width = latent_cache.shape
    seqs, heads, nope = q_nope.shape
    rope_w = q_rope.shape[2]
    cols = w_uk.shape[2]
    vdim = value_up_weight.shape[2]
    scale = (nope + rope_w) ** (-0.5) * math.log2(math.e)
    pack = max(1, min(seqs, 128 // cols))
    lanes = pack * cols
    hs = heads // n
    line = n // 2
    rows = seqs * hs
    wide = w_out.shape[1]
    nch = (slots + seqs * (GROUP - 1)) // GROUP
    nch = -(-nch // UNROLL) * UNROLL
    pw = (nch * GROUP + 127) // 128 * 128
    vm = pl.BlockSpec(memory_space=pltpu.VMEM)
    hbm = pl.BlockSpec(memory_space=pl.ANY)
    dma = pltpu.SemaphoreType.DMA
    vmem = pltpu.VMEM
    bulk = 8
    return pl.pallas_call(
        functools.partial(kernel, n, groups, pack, scale, nch),
        out_shape=jax.ShapeDtypeStruct((seqs, wide // 2), BF16),
        in_specs=[hbm] * 9, out_specs=vm,
        scratch_shapes=[
            pltpu.SMEM(lengths.shape, jnp.int32),
            vmem(page_table.shape, jnp.int32),
            vmem(rope_cache.shape, BF16),
            vmem(q_nope.shape, BF16),
            vmem((heads, cols, nope), BF16),
            vmem(q_rope.shape, BF16),
            vmem((2, slots, page, width // 2), BF16),
            vmem(w_out.shape, BF16),
            vmem((8, pw), jnp.int32),
            pltpu.SMEM((8, pw), jnp.int32),
            vmem((heads * seqs, cols), F32),
            vmem((heads * seqs, nope), F32),
            vmem((n, QPARTS, seqs // pack * heads // QPARTS, lanes), BF16),
            vmem((seqs, heads, width // 2), BF16),
            vmem((seqs, heads, width // 2), BF16),
            vmem((seqs, heads, 128), BF16),
            vmem((slots * (page + 8), 128), F32),
            vmem((slots, page, 128), BF16),
            vmem((2, nch + 1, heads, width // 2), F32),
            vmem((nch + 1, heads, 128), F32),
            vmem((nch + 1, heads, 128), F32),
            vmem((seqs, heads, 128), F32),
            vmem((nch, heads, GROUP * page), F32),
            vmem((nch, heads, GROUP * page), BF16),
            vmem((2, n, rows, width // 2), BF16),
            vmem((n, 2 * hs, 128), F32),
            vmem((2, line, rows, width // 2), BF16),
            vmem((line, 2 * hs, 128), F32),
            vmem((2, line, rows, width // 2), BF16),
            vmem((line, 2 * hs, 128), F32),
            vmem((2, line, rows, width // 2), BF16),
            vmem((line, 2 * hs, 128), F32),
            vmem((width // 128, rows, 128), F32),
            vmem((n, hs, cols, vdim), BF16),
            vmem((n, seqs, hs * vdim), BF16),
            vmem((seqs, wide // 2), F32),
            vmem((seqs, wide // 2), F32),
            dma((7 + QPARTS,)), dma((2 * bulk,)),
            dma((QPARTS * line,)), dma((QPARTS * line,)), dma((QPARTS * line,)), dma((QPARTS * line,)),
            dma((n,)), dma((n,)), dma((n,)), dma((n,)),
            dma((2 * line,)), dma((2 * line,)), dma((line,)), dma((line,)),
            dma((2 * line,)), dma((2 * line,)), dma((line,)), dma((line,)),
            dma((n,)), dma((n,)), dma, dma,
        ],
        compiler_params=pltpu.CompilerParams(
            has_side_effects=True, collective_id=1, vmem_limit_bytes=55216 * 1024),
        name="decode",
    )(lengths, page_table, rope_cache, q_nope, w_uk.transpose(0, 2, 1), q_rope, latent_cache, value_up_weight, w_out)


def solution(mesh):
    return jax.shard_map(
        functools.partial(local, mesh.shape["seq"], mesh.shape["groups"]),
        mesh=mesh,
        in_specs=(
            P(("groups", "seq"), None, None),
            P(("groups", "seq"), None),
            P("groups", "mp", None),
            P("groups", "mp", None),
            P("mp", None, "seq"),
            P("mp", "seq", None),
            P("mp", "seq"),
            P("groups", None),
            P("groups"),
        ),
        out_specs=P("groups", ("seq", "mp")),
        check_vma=False,
    )
```

```python
import functools
import math

import jax
import jax.numpy as jnp
from jax import lax
from jax.experimental import pallas as pl
from jax.experimental.pallas import tpu as pltpu
from jax.sharding import PartitionSpec as P

NEG = -1e30
MESH = pl.DeviceIdType.MESH
GROUP = 4
UNROLL = 38
UNROLL1 = 19
QPARTS = 2
F32 = jnp.float32
BF16 = jnp.bfloat16


def make_plan(first_slot, page, lengths_ref, table_ref, plan_ref):
    seqs, pages = table_ref.shape
    slots_dev, wide = first_slot[1], plan_ref.shape[1]
    table = table_ref[...].astype(F32).T
    logical = lax.broadcasted_iota(jnp.int32, (pages, 1), 0)
    slot = lax.broadcasted_iota(jnp.int32, (pages, slots_dev), 1) + first_slot[0]
    slot = slot.astype(F32)
    fill = []
    for b in range(seqs):
        inside = jnp.clip(lengths_ref[b] - page * logical, 0, page)
        hit = table[:, b:b + 1] == slot
        fill.append(jnp.sum(jnp.where(hit, inside, 0), axis=0, keepdims=True))
    eye = (lax.broadcasted_iota(jnp.int32, (slots_dev, slots_dev), 0)
           == lax.broadcasted_iota(jnp.int32, (slots_dev, slots_dev), 1))
    earlier = (lax.broadcasted_iota(jnp.int32, (slots_dev, slots_dev), 1)
               < lax.broadcasted_iota(jnp.int32, (slots_dev, slots_dev), 0))
    at = lax.broadcasted_iota(jnp.int32, (1, wide), 1)
    start = jnp.zeros((1, 1), jnp.int32)
    owner = jnp.zeros((1, wide), jnp.int32)
    fresh = jnp.zeros((1, wide), jnp.int32)
    entry = jnp.zeros((1, wide), jnp.int32)
    target = jnp.full((slots_dev, 1), -1, jnp.int32)
    column = jnp.zeros((slots_dev, 1), jnp.int32)
    for b in range(seqs):
        owned = fill[b] > 0
        count = jnp.sum(owned.astype(jnp.int32), axis=1, keepdims=True)
        place = jnp.sum(jnp.where(earlier & owned, 1, 0), axis=1, keepdims=True)
        mine = jnp.sum(jnp.where(eye, fill[b], 0), axis=1, keepdims=True)
        target = jnp.where(mine > 0, start * GROUP + place, target)
        column = column + mine
        fresh = jnp.where(at == start, 1, fresh)
        start = start + (count + GROUP - 1) // GROUP
        owner = owner + (at >= start).astype(jnp.int32)
        entry = jnp.where((at == b) & (count > 0), start, entry)
    match = target == lax.broadcasted_iota(jnp.int32, (slots_dev, wide), 1)
    ids = lax.broadcasted_iota(jnp.int32, (slots_dev, wide), 0)
    plan_ref[0:1, :] = jnp.sum(jnp.where(match, ids, 0), axis=0, keepdims=True)
    plan_ref[1:2, :] = jnp.sum(jnp.where(match, column, 0), axis=0, keepdims=True)
    plan_ref[2:3, :] = jnp.minimum(owner, seqs - 1)
    plan_ref[3:4, :] = fresh
    plan_ref[4:5, :] = entry
    plan_ref[5:8, :] = jnp.zeros((3, wide), jnp.int32)


def weigh(seqs, stats):
    hs = stats[0].shape[0] // 2
    tops = [s[:hs] for s in stats]
    best = functools.reduce(jnp.maximum, tops)
    shares = [s[hs:] * jnp.exp2(t - best) for s, t in zip(stats, tops)]
    total = functools.reduce(jnp.add, shares)
    inv = 1.0 / jnp.maximum(total, 1e-30)
    columns = []
    for share in shares:
        share = share * inv
        columns.append(jnp.concatenate([share[:, b:b + 1] for b in range(seqs)], axis=0))
    return columns, best, total


def mean(columns, parts):
    return functools.reduce(jnp.add, [p.astype(F32) * c for c, p in zip(columns, parts)])


def kernel(n, groups, pack, scale, nch,
           lengths_hbm, table_hbm, rope_hbm, qn_hbm, wuk_hbm, qr_hbm, lat_hbm, v_hbm, w_hbm, out_ref,
           lengths, table, rope, qn, wuk, qr, lat, w_buf, plan_v, plan, raw, flat, gath, q_near, q_far, turn,
           wide_rope, spread, run, tops, sums, peak, part, wts, mix, st, ygot, yst, zout, zst, zgot, zgst, port,
           vbuf, vals, tx, rx,
           lsem, bulk, qs1, qr1, qs2, qr2, vs1, vr1, vs2, vr2, ys, yr, yss, ysr, zs, zr, zss, zsr, as_, ar, ms, mr):
    me = lax.axis_index("seq")
    half = lax.axis_index("mp")
    grp = lax.axis_index("groups")
    seqs, heads, _ = qn.shape
    cols = wuk.shape[1]
    _, slots, page, wing = lat.shape
    width = 2 * wing
    hs = heads // n
    line = n // 2
    par = lax.rem(me, 2)
    row = me // 2
    partner = me + 1 - 2 * par
    share = groups == 2 and hs % 2 == 0
    hh = hs // 2 if share else hs
    voff = grp * hh if share else 0
    hp = heads // QPARTS
    near_n = line // 2
    side, pos = row // near_n, lax.rem(row, near_n)

    def along_of(j, sign):
        other, k = (0, j) if j < near_n else (1, j - near_n)
        at = lax.rem(pos + sign * k + near_n, near_n)
        return 2 * ((side + other * (1 - 2 * side)) * near_n + at) + par

    rows_out = []
    for j in range(line - 1):
        down = jnp.where(line - 1 - j > row, line - 1 - j, line - 2 - j)
        rows_out.append(jnp.where(side == 0, down, jnp.where(row > j, j, j + 1)))
    peers = [2 * r + par for r in rows_out] + [2 * r + 1 - par for r in rows_out] + [partner]

    barrier = pltpu.get_barrier_semaphore()
    for k in range(1, n):
        pl.semaphore_signal(barrier, inc=1, device_id={"seq": lax.rem(me + k, n)}, device_id_type=MESH)
    pl.semaphore_signal(barrier, inc=1, device_id={"mp": 1 - half}, device_id_type=MESH)
    if share:
        pl.semaphore_signal(barrier, inc=1, device_id={"groups": 1 - grp}, device_id_type=MESH)

    loads = [pltpu.make_async_copy(a, b, lsem.at[i]) for i, (a, b) in enumerate((
        (qn_hbm, qn), (wuk_hbm.at[pl.ds(0, hp)], wuk.at[pl.ds(0, hp)]), (lengths_hbm, lengths), (table_hbm, table), (qr_hbm, qr), (rope_hbm, rope)) + tuple(
            (wuk_hbm.at[pl.ds(i * hp, hp)], wuk.at[pl.ds(i * hp, hp)]) for i in range(1, QPARTS)))]
    for i in (0, 1, *range(6, len(loads)), 2, 3, 4, 5):
        loads[i].start()
    nb = bulk.shape[0] // 2
    step_l = 2 * slots // nb
    big = [pltpu.make_async_copy(
        lat_hbm.at[pl.ds(i // 2 * step_l, step_l), :, pl.ds(i % 2 * wing, wing)],
        lat.at[i % 2, pl.ds(i // 2 * step_l, step_l)], bulk.at[i]) for i in range(nb)]
    step_w = w_buf.shape[0] // nb
    bigw = [pltpu.make_async_copy(w_hbm.at[pl.ds(i * step_w, step_w)], w_buf.at[pl.ds(i * step_w, step_w)], bulk.at[nb + i])
            for i in range(nb)]
    own_v = pltpu.make_async_copy(v_hbm.at[pl.ds(me * hs, hs)], vbuf.at[me], lsem.at[5 + QPARTS])

    def remote(src, dst, s, r, where):
        return pltpu.make_async_remote_copy(
            src_ref=src, dst_ref=dst, send_sem=s, recv_sem=r, device_id=where, device_id_type=MESH)

    loads[0].wait()
    for b in range(seqs):
        flat[b * heads:(b + 1) * heads, :] = qn[b].astype(F32)

    def q_copy(block, i, k, peer, s, r):
        return remote(gath.at[block, i], gath.at[block, i], s.at[i * line + k], r.at[i * line + k], {"seq": peer})

    along, across = [], []
    for i in range(QPARTS):
        loads[5 + i if i else 1].wait()
        if i == QPARTS - 1:
            for copy in big:
                copy.start()
        for h in range(i * hp, (i + 1) * hp):
            q = flat[pl.ds(h, seqs, stride=heads), :].astype(BF16)
            raw[h * seqs:(h + 1) * seqs, :] = lax.dot_general(
                q, wuk[h], (((1,), (1,)), ((), ())), preferred_element_type=F32)
        for p in range(seqs // pack):
            parts = [raw[pl.ds(i * hp * seqs + p * pack + j, hp, stride=seqs), :] for j in range(pack)]
            whole = parts[0] if pack == 1 else jnp.concatenate(parts, axis=1)
            gath[me, i, p * hp:(p + 1) * hp, :] = whole.astype(BF16)
        if i == 0:
            pl.semaphore_wait(barrier, n - 1 + 1 + int(share))
        for k in range(1, line):
            copy = q_copy(me, i, k, along_of(k, 1), qs1, qr1)
            copy.start()
            along.append((i, k, copy))
        copy = q_copy(me, i, 0, partner, qs2, qr2)
        copy.start()
        across.append((0, copy))

    def v_copy(d, s):
        return remote(v_hbm.at[pl.ds(d * hs + voff, hh)], vbuf.at[s, pl.ds(voff, hh)], vs1.at[d], vr1.at[s], {"seq": d})

    def twin_copy(s):
        return remote(vbuf.at[s, pl.ds(voff, hh)], vbuf.at[s, pl.ds(voff, hh)], vs2.at[s], vr2.at[s], {"groups": 1 - grp})

    def relay(sources):
        for s in sources if share else []:
            v_copy(s, s).wait_recv()
            twin_copy(s).start()

    loads[2].wait()
    loads[3].wait()
    make_plan((me * slots, slots), page, lengths, table, plan_v)
    plan_copy = pltpu.make_async_copy(plan_v, plan, lsem.at[6 + QPARTS])
    plan_copy.start()
    loads[4].wait()
    loads[5].wait()
    own_v.start()
    per = page * 128 // rope.shape[1]
    pitch = wide_rope.shape[0] // slots
    lane = lax.broadcasted_iota(jnp.int32, (slots, 128), 1) // (128 // per)

    def widen(i):
        x = rope[:, i * 128:(i + 1) * 128].astype(F32)
        for j in range(per):
            wide_rope[pl.ds(i * per + j, slots, stride=pitch), :] = jnp.where(lane == j, x, 0.0)

    def narrow(i, _):
        spread[i] = wide_rope[pl.ds(pl.multiple_of(i * pitch, 8), page), :].astype(BF16)
        return 0

    along.sort(key=lambda x: (x[1] >= near_n, x[0], x[1]))
    steps = rope.shape[1] // 128
    share_w = -(-steps // max(1, len(along) // 2))
    for i, (q, k, copy) in enumerate(along):
        for f in range(min(steps, i * share_w), min(steps, (i + 1) * share_w)):
            widen(f)
        if (i + 1) * share_w >= steps > i * share_w:
            lax.fori_loop(0, slots, narrow, 0, unroll=4)
        copy.wait_recv()
        forward = q_copy(along_of(k, -1), q, k, partner, qs2, qr2)
        forward.start()
        across.append((k, forward))

    for d in peers:
        v_copy(d, me).start()

    for b in range(seqs):
        turn[b] = jnp.concatenate([qr[b]] * (128 // qr.shape[2]), axis=1)
    for j in range(2):
        run[j, 0] = jnp.zeros(run.shape[2:], F32)
    tops[0] = jnp.full(tops.shape[1:], NEG, F32)
    sums[0] = jnp.zeros(sums.shape[1:], F32)
    plan_copy.wait()
    for copy in big:
        copy.wait()
    for copy in bigw:
        copy.start()

    def assemble(first, dst):
        for i in range(QPARTS):
            for s in range(n // 2):
                for b in range(seqs):
                    at = b % pack * cols
                    dst[b, i * hp:(i + 1) * hp, s * cols:(s + 1) * cols] = gath[
                        first + s, i, b // pack * hp:(b // pack + 1) * hp, at:at + cols]

    tokens = GROUP * page
    tlane = lax.broadcasted_iota(jnp.int32, (1, tokens), 1)
    nt = (((1,), (1,)), ((), ()))

    def slots_of(ref, c):
        return jnp.concatenate([ref[plan[0, c * GROUP + g]] for g in range(GROUP)], axis=0)

    def first_pass(it, _):
        for u in range(UNROLL1):
            c = it * UNROLL1 + u
            b = plan[2, c]
            limit = jnp.zeros((1, tokens), jnp.int32)
            for g in range(GROUP):
                limit = jnp.where(tlane // page == g, plan[1, c * GROUP + g] + g * page, limit)
            score = lax.dot_general(turn[b], slots_of(spread, c), nt, preferred_element_type=F32)
            score = score + lax.dot_general(q_near[b], slots_of(lat.at[side], c), nt, preferred_element_type=F32)
            part[c] = jnp.where(tlane < limit, score, NEG)
        return 0

    for k, copy in across:
        if k < near_n:
            copy.wait_recv()
    assemble(side * (n // 2), q_near)
    trips = nch // UNROLL
    lax.fori_loop(0, nch // UNROLL1, first_pass, 0)
    for k, copy in across:
        if k >= near_n:
            copy.wait_recv()
    assemble((1 - side) * (n // 2), q_far)

    def second_pass(it, _):
        top = tops[it * UNROLL]
        for u in range(UNROLL):
            c = it * UNROLL + u
            far = lax.dot_general(q_far[plan[2, c]], slots_of(lat.at[1 - side], c), nt, preferred_element_type=F32)
            score = (part[c] + far) * scale
            part[c] = score
            top = jnp.where(plan[3, c] > 0, NEG, top)
            for j in range(tokens // 128):
                top = jnp.maximum(top, score[:, j * 128:(j + 1) * 128])
            tops[c + 1] = top
        return 0

    lax.fori_loop(0, trips, second_pass, 0)
    for b in range(seqs):
        peak[b] = jnp.broadcast_to(jnp.max(tops[plan[4, b]], axis=1, keepdims=True), peak.shape[1:])

    def third_pass(it, _):
        acc, total = run[0, it * UNROLL], sums[it * UNROLL]
        for u in range(UNROLL):
            c = it * UNROLL + u
            top = peak[plan[2, c]]
            keep = jnp.where(plan[3, c] > 0, 0.0, 1.0)
            weight = [jnp.exp2(part[c, :, j * 128:(j + 1) * 128] - top) for j in range(tokens // 128)]
            total = total * keep + functools.reduce(jnp.add, weight)
            weight = jnp.concatenate([x.astype(BF16) for x in weight], axis=1)
            wts[c] = weight
            acc = acc * keep + jnp.dot(weight, slots_of(lat.at[0], c), preferred_element_type=F32)
            sums[c + 1] = total
            run[0, c + 1] = acc
        return 0

    def fourth_pass(it, _):
        acc = run[1, it * UNROLL]
        for u in range(UNROLL):
            c = it * UNROLL + u
            keep = jnp.where(plan[3, c] > 0, 0.0, 1.0)
            acc = acc * keep + jnp.dot(wts[c], slots_of(lat.at[1], c), preferred_element_type=F32)
            run[1, c + 1] = acc
        return 0

    ids = lax.broadcasted_iota(jnp.int32, (heads, 128), 1)
    everyone = rows_out + [row]

    def pack_sums(j):
        all_top = jnp.full((heads, 128), NEG, F32)
        all_sum = jnp.zeros((heads, 128), F32)
        for p in range(seqs // 2):
            pair = []
            for b in (2 * p, 2 * p + 1):
                entry = plan[4, b]
                total = jnp.sum(sums[entry], axis=1, keepdims=True)
                all_top = jnp.where(ids == b, peak[b], all_top)
                all_sum = jnp.where(ids == b, total, all_sum)
                pair.append(run[j, entry] * (1.0 / jnp.maximum(total, 1e-30)))
            for d in range(n):
                mix[j, d, 2 * p * hs:2 * (p + 1) * hs, :] = jnp.concatenate(
                    [x[d * hs:(d + 1) * hs] for x in pair], axis=0).astype(BF16)
        if j == 0:
            for d in range(n):
                st[d, :hs, :] = all_top[d * hs:(d + 1) * hs]
                st[d, hs:, :] = all_sum[d * hs:(d + 1) * hs]

    ysent = {}

    def to_partner(j, places):
        for i in places:
            r = everyone[i]
            d = 2 * r + 1 - par
            if j == 0:
                ysent[2, i] = remote(st.at[d], yst.at[r], yss.at[i], ysr.at[i], {"seq": partner})
                ysent[2, i].start()
            ysent[j, i] = remote(mix.at[j, d], ygot.at[j, r], ys.at[j * line + i], yr.at[j * line + i], {"seq": partner})
            ysent[j, i].start()

    lax.fori_loop(0, trips, third_pass, 0)
    pack_sums(0)
    to_partner(0, range(line - 1))
    relay(peers[:line - 1][::-1])
    lax.fori_loop(0, trips, fourth_pass, 0)
    pack_sums(1)
    to_partner(1, range(line - 1))
    to_partner(0, [line - 1])
    to_partner(1, [line - 1])
    onward = []
    for j, i in [(j, i) for j in range(2) for i in range(line - 1)] + [(0, line - 1), (1, line - 1)]:
        r = everyone[i]
        if j == 0:
            ysent[2, i].wait_recv()
        ysent[j, i].wait_recv()
        mine = 2 * r + par
        columns, best, total = weigh(seqs, [st[mine], yst[r]])
        zout[j, i] = mean(columns, [mix[j, mine], ygot[j, r]]).astype(BF16)
        moves = [(zout.at[j, i], zgot.at[j, row], zs.at[j * line + i], zr.at[j * line + row])]
        if j == 0:
            zst[i, :hs, :] = best
            zst[i, hs:, :] = total
            moves.append((zst.at[i], zgst.at[row], zss.at[i], zsr.at[row]))
        if i < line - 1:
            for move in moves:
                copy = remote(*move, {"seq": 2 * r + par})
                copy.start()
                onward.append(copy)
        relay(peers[line - 1:][i + j * (line - 1):i + j * (line - 1) + 1] if i < line - 1 else [])
    blocks = wing // 128
    for j in range(2):
        for r in rows_out:
            if j == 0:
                remote(zst.at[0], zgst.at[r], zss.at[0], zsr.at[r], {"seq": partner}).wait_recv()
            remote(zout.at[j, 0], zgot.at[j, r], zs.at[0], zr.at[j * line + r], {"seq": partner}).wait_recv()
        columns, _, _ = weigh(seqs, [zst[line - 1]] + [zgst[r] for r in rows_out])
        o = mean(columns, [zout[j, line - 1]] + [zgot[j, r] for r in rows_out])
        for i in range(blocks):
            port[j * blocks + i] = o[:, i * 128:(i + 1) * 128]

    own_v.wait()
    for d in peers:
        if share:
            twin_copy(d).wait_recv()
        else:
            v_copy(d, d).wait_recv()
    vdim = vbuf.shape[3]
    for h in range(hs):
        x = jnp.concatenate([port[j, pl.ds(h, seqs, stride=hs), :] for j in range(2 * blocks)], axis=1).astype(BF16)
        wv = vbuf[:, h].reshape(width, vdim)
        vals[me, :, h * vdim:(h + 1) * vdim] = jnp.dot(x, wv, preferred_element_type=F32).astype(BF16)
    copies = []
    for i in [x for j in range(line - 1) for x in (line - 1 + j, j)] + [n - 2]:
        copy = remote(vals.at[me], vals.at[me], as_.at[i], ar.at[me], {"seq": peers[i]})
        copy.start()
        copies.append(copy)
    for copy in bigw:
        copy.wait()
    rows = hs * vdim
    res = None
    for src in [me, partner] + [peers[i] for j in range(line - 2, -1, -1) for i in (j, line - 1 + j)]:
        if src is not me:
            remote(vals.at[src], vals.at[src], as_.at[0], ar.at[src], {"seq": partner}).wait_recv()
        at = pl.ds(pl.multiple_of(src * rows, rows), rows)
        product = jnp.dot(vals[src], w_buf[at, :], preferred_element_type=F32)
        res = product if res is None else res + product
    wide = res.shape[1] // 2
    low, high = res[:, :wide], res[:, wide:]
    first = half == 0
    tx[...] = jnp.where(first, high, low)
    copy = remote(tx, rx, ms, mr, {"mp": 1 - half})
    copy.start()
    for c in copies + list(ysent.values()) + onward + [x[2] for x in along] + [x[1] for x in across]:
        c.wait_send()
    for d in peers:
        v_copy(d, me).wait_send()
        if share:
            twin_copy(d).wait_send()
    copy.wait()
    out_ref[...] = (jnp.where(first, low, high) + rx[...]).astype(BF16)


def local(n, groups, latent_cache, rope_cache, q_nope, q_rope, w_uk, value_up_weight, w_out, page_table, lengths):
    slots, page, width = latent_cache.shape
    seqs, heads, nope = q_nope.shape
    rope_w = q_rope.shape[2]
    cols = w_uk.shape[2]
    vdim = value_up_weight.shape[2]
    scale = (nope + rope_w) ** (-0.5) * math.log2(math.e)
    pack = max(1, min(seqs, 128 // cols))
    lanes = pack * cols
    hs = heads // n
    line = n // 2
    rows = seqs * hs
    wide = w_out.shape[1]
    nch = (slots + seqs * (GROUP - 1)) // GROUP
    nch = -(-nch // UNROLL) * UNROLL
    pw = (nch * GROUP + 127) // 128 * 128
    vm = pl.BlockSpec(memory_space=pltpu.VMEM)
    hbm = pl.BlockSpec(memory_space=pl.ANY)
    dma = pltpu.SemaphoreType.DMA
    vmem = pltpu.VMEM
    bulk = 8
    return pl.pallas_call(
        functools.partial(kernel, n, groups, pack, scale, nch),
        out_shape=jax.ShapeDtypeStruct((seqs, wide // 2), BF16),
        in_specs=[hbm] * 9, out_specs=vm,
        scratch_shapes=[
            pltpu.SMEM(lengths.shape, jnp.int32),
            vmem(page_table.shape, jnp.int32),
            vmem(rope_cache.shape, BF16),
            vmem(q_nope.shape, BF16),
            vmem((heads, cols, nope), BF16),
            vmem(q_rope.shape, BF16),
            vmem((2, slots, page, width // 2), BF16),
            vmem(w_out.shape, BF16),
            vmem((8, pw), jnp.int32),
            pltpu.SMEM((8, pw), jnp.int32),
            vmem((heads * seqs, cols), F32),
            vmem((heads * seqs, nope), F32),
            vmem((n, QPARTS, seqs // pack * heads // QPARTS, lanes), BF16),
            vmem((seqs, heads, width // 2), BF16),
            vmem((seqs, heads, width // 2), BF16),
            vmem((seqs, heads, 128), BF16),
            vmem((slots * (page + 8), 128), F32),
            vmem((slots, page, 128), BF16),
            vmem((2, nch + 1, heads, width // 2), F32),
            vmem((nch + 1, heads, 128), F32),
            vmem((nch + 1, heads, 128), F32),
            vmem((seqs, heads, 128), F32),
            vmem((nch, heads, GROUP * page), F32),
            vmem((nch, heads, GROUP * page), BF16),
            vmem((2, n, rows, width // 2), BF16),
            vmem((n, 2 * hs, 128), F32),
            vmem((2, line, rows, width // 2), BF16),
            vmem((line, 2 * hs, 128), F32),
            vmem((2, line, rows, width // 2), BF16),
            vmem((line, 2 * hs, 128), F32),
            vmem((2, line, rows, width // 2), BF16),
            vmem((line, 2 * hs, 128), F32),
            vmem((width // 128, rows, 128), F32),
            vmem((n, hs, cols, vdim), BF16),
            vmem((n, seqs, hs * vdim), BF16),
            vmem((seqs, wide // 2), F32),
            vmem((seqs, wide // 2), F32),
            dma((7 + QPARTS,)), dma((2 * bulk,)),
            dma((QPARTS * line,)), dma((QPARTS * line,)), dma((QPARTS * line,)), dma((QPARTS * line,)),
            dma((n,)), dma((n,)), dma((n,)), dma((n,)),
            dma((2 * line,)), dma((2 * line,)), dma((line,)), dma((line,)),
            dma((2 * line,)), dma((2 * line,)), dma((line,)), dma((line,)),
            dma((n,)), dma((n,)), dma, dma,
        ],
        compiler_params=pltpu.CompilerParams(
            has_side_effects=True, collective_id=1, vmem_limit_bytes=55216 * 1024),
        name="decode",
    )(lengths, page_table, rope_cache, q_nope, w_uk.transpose(0, 2, 1), q_rope, latent_cache, value_up_weight, w_out)


def solution(mesh):
    return jax.shard_map(
        functools.partial(local, mesh.shape["seq"], mesh.shape["groups"]),
        mesh=mesh,
        in_specs=(
            P(("groups", "seq"), None, None),
            P(("groups", "seq"), None),
            P("groups", "mp", None),
            P("groups", "mp", None),
            P("mp", None, "seq"),
            P("mp", "seq", None),
            P("mp", "seq"),
            P("groups", None),
            P("groups"),
        ),
        out_specs=P("groups", ("seq", "mp")),
        check_vma=False,
    )
```
